32 devices in a mesh: seq: 8 (over z, y), tensor: 4 (over x, core).
Axes of the slice: x: 2, y: 2, z: 4, core: 2. Of those that a mesh axis runs over, the one named last changes fastest.
Arguments:
- fixed_point: bfloat16 [1024, 4096], P(('seq', 'tensor')), may hold values from -6 to 6
- incoming: bfloat16 [1024, 4096], P(('seq', 'tensor')), may hold values from -6 to 6
- norm_gain: float32 [4096], replicated, may hold values from 0.1 to 1.9
- query_weight: bfloat16 [4096, 4096], P(None, 'tensor'), may hold values from -0.21875 to 0.21875, as said below
- key_weight: bfloat16 [4096, 4096], P(None, 'tensor'), may hold values from -0.265625 to 0.265625, as said below
- value_weight: bfloat16 [4096, 4096], P(None, 'tensor'), may hold values from -0.09375 to 0.09375
- out_weight: bfloat16 [4096, 4096], P('tensor'), may hold values from -0.09375 to 0.09375
- layout: int32 [16, 16], replicated, may hold values 0 or 1
Outputs:
- adjoint: float32 [1024, 4096], P(('seq', 'tensor'))
- gain_grad: float32 [4096], replicated
The draws below stay inside these ranges and needn't reach their ends.
Inputs may be any that keep to these rules, and one draw needn't show every extreme that they name: `query_weight`: entries of the columns of each head are independent; their spread may differ between heads. `key_weight`: entries are independent within a draw; columns of some heads may follow the same head's columns of query_weight. `layout`: A key block strictly before a query block is attended where the entry at row query block, column key block is 1; a block always attends itself causally; entries on or above the diagonal are not read.
All inputs are finite; a program needn't handle non-finite values.
Results may differ from the reference program's by a relative error of at most 0.03.
Values may be sent and summed in bfloat16 or wider, within the bound.
No kernel may reach another device: no remote copies, remote signals or barrier semaphores. Data moves between devices by JAX's collectives and lax.ppermute only.
A program may use at most 128 MiB of HBM per device.

```python
import jax
import jax.numpy as jnp
from jax import lax

D = 4096
HEADS = 32
HEAD_DIM = 128
BLK = 64
ITERS = 2
HEADS_DEV = 8
LENGTH = 1024
NBLK = 16


def projection_pair(key):
    first = jax.random.truncated_normal(jax.random.fold_in(key, 11), -4.0, 4.0, (D, D), jnp.float32)
    second = jax.random.truncated_normal(jax.random.fold_in(key, 23), -4.0, 4.0, (D, D), jnp.float32)
    plain = (2.0 / D) ** 0.5
    query = first * plain
    keyed = second * plain
    return (query, keyed)


def draw_query_weight(key, part):
    return projection_pair(key)[0].astype(jnp.bfloat16)


def draw_key_weight(key, part):
    return projection_pair(key)[1].astype(jnp.bfloat16)


def set_ends(values, stream_key, least, top_value):
    shape = values.shape
    place = [jax.random.randint(jax.random.fold_in(stream_key, axis), (), 0, shape[axis]) for axis in range(len(shape))]
    values = values.at[tuple(place)].set(least)
    longest = shape.index(max(shape))
    place[longest] = (place[longest] + 1) % shape[longest]
    return values.at[tuple(place)].set(top_value)


def block_levels(own_key, shape, cuts, smallest, top_value):
    def one(dim, parts):
        heights = jax.random.uniform(jax.random.fold_in(jax.random.fold_in(own_key, 6), dim), (parts,), jnp.float32, smallest / len(cuts), top_value / len(cuts))
        return jnp.repeat(jnp.exp(heights), shape[dim] // parts).reshape((-1,) + (1,) * (len(shape) - dim - 1))

    loudness = one(*cuts[0])
    for cut in cuts[1:]:
        loudness = loudness * one(*cut)
    return loudness


def noise(stream_key, dims, scale, bound, cuts=(), kind=jnp.bfloat16):
    values = scale * jax.random.normal(stream_key, dims, jnp.float32)
    if cuts:
        values = values * block_levels(stream_key, dims, cuts, -0.22, 0.18)
    return jnp.clip(values, -bound, bound).astype(kind)


def setup_inputs(seed: int = 0) -> dict:
    splits = jax.random.split(jax.random.key(seed), 9)
    fixed_point = noise(splits[0], (LENGTH, D), 1.0, 6.0, ((0, 32),))
    incoming = noise(splits[1], (LENGTH, D), 1.0, 6.0, ((0, 32),))
    norm_gain = jnp.clip(1.0 + 0.18 * jax.random.normal(splits[2], (D,), jnp.float32), 0.1, 1.9)
    query_weight = draw_query_weight(jax.random.fold_in(splits[8], 71), 0)
    key_weight = draw_key_weight(jax.random.fold_in(splits[8], 71), 0)
    value_weight = noise(splits[5], (D, D), D ** -0.5, 0.09375, ((1, 4),))
    out_weight = noise(splits[6], (D, D), D ** -0.5, 0.09375, ((0, 4),))
    layout = set_ends((jax.random.randint(splits[7], (NBLK, NBLK), 0, 4) < 3).astype(jnp.int32), jax.random.fold_in(splits[7], 1), 0, 1)
    return dict(fixed_point=fixed_point, incoming=incoming, norm_gain=norm_gain, query_weight=query_weight, key_weight=key_weight, value_weight=value_weight, out_weight=out_weight, layout=layout)


EPS = 1e-05
THETA = 10000.0
MASKED = -1e+30

def round_low(values):
    return lax.optimization_barrier(values.astype(jnp.bfloat16)).astype(jnp.float32)

def rope_tables(positions):
    freq = THETA ** (-jnp.arange(0, HEAD_DIM, 2, dtype=jnp.float32) / HEAD_DIM)
    angle = positions.astype(jnp.float32)[:, None] * freq[None, :]
    cosine = jnp.concatenate([jnp.cos(angle), jnp.cos(angle)], axis=1)[:, None, :]
    sine = jnp.concatenate([jnp.sin(angle), jnp.sin(angle)], axis=1)[:, None, :]
    return (cosine, sine)

def rotate(values, cosine, sine):
    half = HEAD_DIM // 2
    turned = jnp.concatenate([-values[..., half:], values[..., :half]], axis=-1)
    return values * cosine + turned * sine

def rotate_back(values, cosine, sine):
    half = HEAD_DIM // 2
    weighted = values * sine
    turned = jnp.concatenate([weighted[..., half:], -weighted[..., :half]], axis=-1)
    return values * cosine + turned

def expand_blocks(chosen):
    return jnp.repeat(jnp.repeat(chosen, BLK, axis=0), BLK, axis=1)

def pair_mask(query_pos, key_pos, chosen):
    query_block = (query_pos // BLK)[:, None]
    key_block = (key_pos // BLK)[None, :]
    earlier = (key_block < query_block) & chosen
    same = (key_block == query_block) & (key_pos[None, :] <= query_pos[:, None])
    return earlier | same

def reference(fixed_point, incoming, norm_gain, query_weight, key_weight, value_weight, out_weight, layout):
    groups = HEADS // HEADS_DEV
    width = HEADS_DEV * HEAD_DIM
    score_scale = HEAD_DIM ** (-0.5)
    point = fixed_point.astype(jnp.float32)
    inv_rms = lax.rsqrt(lax.optimization_barrier(jnp.mean(point * point, axis=1, keepdims=True)) + EPS)
    scaled = point * inv_rms
    normed = (norm_gain * scaled).astype(jnp.bfloat16)
    positions = jnp.arange(LENGTH, dtype=jnp.int32)
    cosine, sine = rope_tables(positions)

    def project(weight):
        return jnp.dot(normed, weight, preferred_element_type=jnp.float32).reshape(LENGTH, HEADS, HEAD_DIM)

    def split_heads(values):
        return values.reshape(LENGTH, groups, HEADS_DEV, HEAD_DIM).transpose(1, 0, 2, 3)
    queries = split_heads(rotate(project(query_weight), cosine, sine).astype(jnp.bfloat16))
    keys = split_heads(rotate(project(key_weight), cosine, sine).astype(jnp.bfloat16))
    values = split_heads(project(value_weight).astype(jnp.bfloat16))
    allowed = pair_mask(positions, positions, expand_blocks(layout > 0))[None]

    def probabilities(query_group, key_group):
        scores = jnp.einsum('qhd,khd->hqk', query_group.astype(jnp.float32), key_group.astype(jnp.float32)) * score_scale
        scores = jnp.where(allowed, scores, MASKED)
        return jnp.exp(scores - jax.nn.logsumexp(scores, axis=2, keepdims=True))

    def forward_group(operands):
        query_group, key_group, value_group = operands
        probs = probabilities(query_group, key_group)
        attended = jnp.einsum('hqk,khd->qhd', round_low(probs), value_group.astype(jnp.float32))
        return attended.astype(jnp.bfloat16)
    attended = lax.map(forward_group, (queries, keys, values))
    query_cols = query_weight.reshape(D, groups, width).transpose(1, 0, 2)
    key_cols = key_weight.reshape(D, groups, width).transpose(1, 0, 2)
    value_cols = value_weight.reshape(D, groups, width).transpose(1, 0, 2)
    out_rows = out_weight.reshape(groups, width, D)

    def backprop(cotangent):
        cotangent_low = cotangent.astype(jnp.bfloat16)

        def group_step(total, operands):
            query_group, key_group, value_group, attended_group, query_col, key_col, value_col, out_row = operands
            grad_out = jnp.dot(cotangent_low, out_row.T, preferred_element_type=jnp.float32).astype(jnp.bfloat16)
            grad_wide = grad_out.astype(jnp.float32).reshape(LENGTH, HEADS_DEV, HEAD_DIM)
            delta = lax.optimization_barrier(jnp.sum(grad_wide * attended_group.astype(jnp.float32), axis=2)).T
            probs = probabilities(query_group, key_group)
            grad_probs = jnp.einsum('qhd,khd->hqk', grad_wide, value_group.astype(jnp.float32))
            grad_scores = round_low(probs * (grad_probs - delta[:, :, None]))
            grad_query = jnp.einsum('hqk,khd->qhd', grad_scores, key_group.astype(jnp.float32)) * score_scale
            grad_key = jnp.einsum('hqk,qhd->khd', grad_scores, query_group.astype(jnp.float32)) * score_scale
            grad_value = jnp.einsum('hqk,qhd->khd', round_low(probs), grad_wide)
            query_low = rotate_back(grad_query, cosine, sine).astype(jnp.bfloat16).reshape(LENGTH, width)
            key_low = rotate_back(grad_key, cosine, sine).astype(jnp.bfloat16).reshape(LENGTH, width)
            value_low = grad_value.astype(jnp.bfloat16).reshape(LENGTH, width)
            partial_sum = jnp.dot(query_low, query_col.T, preferred_element_type=jnp.float32)
            partial_sum = partial_sum + jnp.dot(key_low, key_col.T, preferred_element_type=jnp.float32)
            partial_sum = partial_sum + jnp.dot(value_low, value_col.T, preferred_element_type=jnp.float32)
            return (total + round_low(partial_sum), None)
        operands = (queries, keys, values, attended, query_cols, key_cols, value_cols, out_rows)
        grad_normed, _ = lax.scan(group_step, jnp.zeros((LENGTH, D), jnp.float32), operands)
        return grad_normed
    cotangent = incoming.astype(jnp.float32)
    adjoint = cotangent
    gain_total = jnp.zeros((D,), jnp.float32)
    for term_index in range(ITERS):
        grad_normed = backprop(cotangent)
        gain_total = gain_total + lax.optimization_barrier(jnp.sum(grad_normed * scaled, axis=0))
        weighted = norm_gain * grad_normed
        inner = lax.optimization_barrier(jnp.sum(weighted * scaled, axis=1, keepdims=True))
        cotangent = inv_rms * (weighted - scaled * (inner / D))
        adjoint = adjoint + cotangent
    return (adjoint, gain_total * LENGTH ** (-0.5))
```

```python
import functools

import jax
import jax.numpy as jnp
from jax import lax
from jax.experimental import pallas as pl
from jax.experimental.pallas import tpu as pltpu
from jax.sharding import PartitionSpec as P

HEAD_DIM = 128
BLK = 64
ITERS = 2


EPS = 1e-05
THETA = 10000.0
MASKED = -1e30


def rope_tables(positions):
    freq = THETA ** (-jnp.arange(0, HEAD_DIM, 2, dtype=jnp.float32) / HEAD_DIM)
    angle = positions.astype(jnp.float32)[:, None] * freq[None, :]
    cosine = jnp.concatenate([jnp.cos(angle), jnp.cos(angle)], axis=1)[:, None, :]
    sine = jnp.concatenate([jnp.sin(angle), jnp.sin(angle)], axis=1)[:, None, :]
    return (cosine, sine)


def rotate(values, cosine, sine):
    half = HEAD_DIM // 2
    turned = jnp.concatenate([-values[..., half:], values[..., :half]], axis=-1)
    return values * cosine + turned * sine


def rotate_back(values, cosine, sine):
    half = HEAD_DIM // 2
    weighted = values * sine
    turned = jnp.concatenate([weighted[..., half:], -weighted[..., :half]], axis=-1)
    return values * cosine + turned


def expand_blocks(chosen):
    return jnp.repeat(jnp.repeat(chosen, BLK, axis=0), BLK, axis=1)


def pair_mask(query_pos, key_pos, chosen):
    query_block = (query_pos // BLK)[:, None]
    key_block = (key_pos // BLK)[None, :]
    earlier = (key_block < query_block) & chosen
    same = (key_block == query_block) & (key_pos[None, :] <= query_pos[:, None])
    return earlier | same


def gathered_body(
    fixed_point, incoming, norm_gain, query_weight, key_weight, value_weight, out_weight, layout
):
    local_rows, model_width = fixed_point.shape
    head_width = query_weight.shape[1]
    head_count = head_width // HEAD_DIM
    seq_tokens = local_rows * lax.axis_size("tensor")
    seq_length = seq_tokens * lax.axis_size("seq")
    seq_index = lax.axis_index("seq")
    score_scale = HEAD_DIM ** (-0.5)
    contract_last = (((1,), (1,)), ((), ()))
    head_shape = (seq_tokens, head_count, HEAD_DIM)
    point = fixed_point.astype(jnp.float32)
    inv_rms = lax.rsqrt(jnp.mean(point * point, axis=1, keepdims=True) + EPS)
    scaled = point * inv_rms
    normed = (norm_gain * scaled).astype(jnp.bfloat16)
    project_piece = lax.all_gather(normed, "tensor", axis=0, tiled=True)
    projected = jnp.concatenate(
        [
            jnp.dot(project_piece, query_weight, preferred_element_type=jnp.float32),
            jnp.dot(project_piece, key_weight, preferred_element_type=jnp.float32),
            jnp.dot(project_piece, value_weight, preferred_element_type=jnp.float32),
        ],
        axis=1,
    )
    positions = seq_index * seq_tokens + jnp.arange(seq_tokens, dtype=jnp.int32)
    cosine, sine = rope_tables(positions)
    queries = rotate(projected[:, :head_width].reshape(head_shape), cosine, sine).astype(
        jnp.bfloat16
    )
    keys = rotate(
        projected[:, head_width : 2 * head_width].reshape(head_shape), cosine, sine
    ).astype(jnp.bfloat16)
    values = projected[:, 2 * head_width :].reshape(head_shape).astype(jnp.bfloat16)
    block_rows = seq_tokens // BLK
    block_count = seq_length // BLK
    first_block = seq_index * block_rows
    key_positions = jnp.arange(seq_length, dtype=jnp.int32)
    chosen_rows = (
        lax.dynamic_slice(layout, (first_block, jnp.int32(0)), (block_rows, block_count)) > 0
    )
    allowed = pair_mask(positions, key_positions, expand_blocks(chosen_rows))
    keys_all, values_all = (
        lax.all_gather(keys, "seq", axis=0, tiled=True),
        lax.all_gather(values, "seq", axis=0, tiled=True),
    )
    scores = (
        jnp.einsum("qhd,khd->hqk", queries, keys_all, preferred_element_type=jnp.float32)
        * score_scale
    )
    scores = jnp.where(allowed[None], scores, MASKED)
    log_norm = jax.nn.logsumexp(scores, axis=2, keepdims=True)
    probs = jnp.exp(scores - log_norm)
    probs_low = probs.astype(jnp.bfloat16)
    attended = jnp.einsum(
        "hqk,khd->qhd", probs_low, values_all, preferred_element_type=jnp.float32
    ).astype(jnp.bfloat16)
    cotangent = incoming.astype(jnp.float32)
    adjoint = cotangent
    gain_grad = jnp.zeros((model_width,), jnp.float32)
    for term_index in range(ITERS):
        grad_out = lax.dot_general(
            lax.all_gather(cotangent.astype(jnp.bfloat16), "tensor", axis=0, tiled=True),
            out_weight,
            contract_last,
            preferred_element_type=jnp.float32,
        )
        grad_low = grad_out.astype(jnp.bfloat16).reshape(head_shape)
        delta = jnp.sum(grad_low.astype(jnp.float32) * attended.astype(jnp.float32), axis=2)
        grad_probs = jnp.einsum(
            "qhd,khd->hqk", grad_low, values_all, preferred_element_type=jnp.float32
        )
        grad_scores = (probs * (grad_probs - delta.T[:, :, None])).astype(jnp.bfloat16)
        grad_query = (
            jnp.einsum("hqk,khd->qhd", grad_scores, keys_all, preferred_element_type=jnp.float32)
            * score_scale
        )
        key_part = (
            jnp.einsum("hqk,qhd->khd", grad_scores, queries, preferred_element_type=jnp.float32)
            * score_scale
        )
        value_part = jnp.einsum(
            "hqk,qhd->khd", probs_low, grad_low, preferred_element_type=jnp.float32
        )
        key_grads = lax.psum_scatter(
            jnp.concatenate(
                [
                    key_part.reshape(seq_tokens * lax.axis_size("seq"), head_width),
                    value_part.reshape(seq_tokens * lax.axis_size("seq"), head_width),
                ],
                axis=1,
            ).astype(jnp.bfloat16),
            "seq",
            scatter_dimension=0,
            tiled=True,
        ).astype(jnp.float32)
        grad_key = key_grads[:, :head_width].reshape(head_shape)
        grad_value = key_grads[:, head_width:].reshape(head_shape)
        query_low = (
            rotate_back(grad_query, cosine, sine)
            .astype(jnp.bfloat16)
            .reshape(seq_tokens, head_width)
        )
        key_low = (
            rotate_back(grad_key, cosine, sine).astype(jnp.bfloat16).reshape(seq_tokens, head_width)
        )
        value_low = grad_value.astype(jnp.bfloat16).reshape(seq_tokens, head_width)
        total = lax.dot_general(
            query_low, query_weight, contract_last, preferred_element_type=jnp.float32
        )
        total = total + lax.dot_general(
            key_low, key_weight, contract_last, preferred_element_type=jnp.float32
        )
        total = total + lax.dot_general(
            value_low, value_weight, contract_last, preferred_element_type=jnp.float32
        )
        grad_normed = lax.psum_scatter(
            total.astype(jnp.bfloat16), "tensor", scatter_dimension=0, tiled=True
        ).astype(jnp.float32)
        gain_term = jnp.sum(grad_normed * scaled, axis=0)
        gain_grad = gain_grad + lax.psum(gain_term, ("seq", "tensor"))
        weighted = norm_gain * grad_normed
        inner = jnp.sum(weighted * scaled, axis=1, keepdims=True)
        cotangent = inv_rms * (weighted - scaled * (inner / model_width))
        adjoint = adjoint + cotangent
    return (adjoint, gain_grad * seq_length ** (-0.5))


def xor_pairs(axis, distance):
    return [(i, i ^ distance) for i in range(lax.axis_size(axis))]


def xor_gather(block):
    blocks = {0: block}
    distance = lax.axis_size("tensor") // 2
    while distance:
        blocks.update(
            {
                j ^ distance: lax.ppermute(b, "tensor", xor_pairs("tensor", distance))
                for j, b in list(blocks.items())
            }
        )
        distance //= 2
    return [blocks[j] for j in range(len(blocks))]


def xor_reduce_scatter(total):
    size = lax.axis_size("tensor")
    rows = total.shape[0] // size
    held = {j: total[j * rows : (j + 1) * rows] for j in range(size)}
    distance = 1
    while distance < size:
        keep = [j for j in held if not j & distance]
        came = [
            lax.ppermute(
                held[j ^ distance].astype(jnp.bfloat16), "tensor", xor_pairs("tensor", distance)
            )
            for j in keep
        ]
        held = {j: held[j] + c.astype(jnp.float32) for j, c in zip(keep, came)}
        distance *= 2
    return held[0]


def all_sum(values):
    for axis in ("tensor", "seq"):
        distance = 1
        while distance < lax.axis_size(axis):
            values = values + lax.ppermute(values, axis, xor_pairs(axis, distance))
            distance *= 2
    return values


def swap_to_heads(values):
    size = lax.axis_size("seq")
    rows, heads, width = values.shape
    values = values.transpose(1, 0, 2).reshape(size, heads // size, rows, width)
    values = lax.all_to_all(values, "seq", split_axis=0, concat_axis=0, tiled=True)
    return values.transpose(1, 0, 2, 3).reshape(heads // size, size * rows, width)


def swap_to_tokens(values):
    size = lax.axis_size("seq")
    heads, tokens, width = values.shape
    values = values.reshape(heads, size, tokens // size, width).transpose(1, 0, 2, 3)
    values = lax.all_to_all(values, "seq", split_axis=0, concat_axis=0, tiled=True)
    return values.transpose(2, 0, 1, 3).reshape(tokens // size, size * heads * width)


def attention_kernel(
    step, flip_ref, layout_ref, q_ref, k_ref, v_ref, g_ref, cos_ref, sin_ref,
    dq_ref, dk_ref, dv_ref, key_acc, value_acc,
):
    tokens, width = q_ref.shape[1:]
    blocks = layout_ref.shape[0]
    flip = flip_ref[0]
    scale = width ** (-0.5)
    key_t = k_ref[0].astype(jnp.float32).T.astype(jnp.bfloat16)
    value_t = v_ref[0].astype(jnp.float32).T.astype(jnp.bfloat16)
    layout = layout_ref[...].astype(jnp.float32).astype(jnp.bfloat16)
    key_acc[...] = jnp.zeros_like(key_acc)
    value_acc[...] = jnp.zeros_like(value_acc)
    contract = lambda a, b, da, db: lax.dot_general(
        a, b, (((da,), (db,)), ((), ())), preferred_element_type=jnp.float32
    )
    for start in range(0, tokens, step):
        seen = start + step
        query = q_ref[0, start:seen, :]
        grad = g_ref[0, start:seen, :]
        key_pos = lax.broadcasted_iota(jnp.int32, (seen, step), 0) ^ flip
        query_pos = (lax.broadcasted_iota(jnp.int32, (seen, step), 1) + start) ^ flip
        key_hot = (
            lax.broadcasted_iota(jnp.int32, (seen, blocks), 1)
            == (lax.broadcasted_iota(jnp.int32, (seen, blocks), 0) ^ flip) // BLK
        )
        query_hot = (
            lax.broadcasted_iota(jnp.int32, (blocks, step), 0)
            == ((lax.broadcasted_iota(jnp.int32, (blocks, step), 1) + start) ^ flip) // BLK
        )
        key_rows = contract(
            key_hot.astype(jnp.float32).astype(jnp.bfloat16), layout, 1, 1
        ).astype(jnp.bfloat16)
        chosen = contract(
            key_rows, query_hot.astype(jnp.float32).astype(jnp.bfloat16), 1, 0
        )
        key_block, query_block = key_pos // BLK, query_pos // BLK
        allowed = ((key_block < query_block) & (chosen > 0.5)) | (
            (key_block == query_block) & (key_pos <= query_pos)
        )
        scores = contract(k_ref[0, :seen, :], query, 1, 1) * scale
        scores = jnp.where(allowed, scores, MASKED)
        probs = jnp.exp(scores - jnp.max(scores, axis=0, keepdims=True))
        probs = probs / jnp.sum(probs, axis=0, keepdims=True)
        low = probs.astype(jnp.bfloat16)
        attended = contract(value_t[:, :seen], low, 1, 0).astype(jnp.bfloat16).astype(jnp.float32)
        grad_t = grad.astype(jnp.float32).T
        delta = jnp.sum(attended * grad_t, axis=0, keepdims=True)
        grad_probs = contract(v_ref[0, :seen, :], grad, 1, 1)
        grad_scores = (probs * (grad_probs - delta)).astype(jnp.bfloat16)
        value_acc[:seen, :] += contract(low, grad, 1, 0)
        key_acc[:seen, :] += contract(grad_scores, query, 1, 0)
        grad_query = (contract(key_t[:, :seen], grad_scores, 1, 0) * scale).T
        dq_ref[0, start:seen, :] = (
            grad_query * cos_ref[start:seen, :]
            + pltpu.roll(grad_query, width // 2, 1) * sin_ref[start:seen, :]
        ).astype(jnp.bfloat16)
    grad_key = key_acc[...] * scale
    dk_ref[0] = (
        grad_key * cos_ref[...] + pltpu.roll(grad_key, width // 2, 1) * sin_ref[...]
    ).astype(jnp.bfloat16)
    dv_ref[0] = value_acc[...].astype(jnp.bfloat16)


def attention_grads(flip, group, layout, queries, keys, values, grads, cosine, sine):
    heads, tokens, width = queries.shape
    step = min(max(256, group), tokens)
    head = pl.BlockSpec((1, tokens, width), lambda h: (h, 0, 0))
    whole = pl.BlockSpec((tokens, width), lambda h: (0, 0))
    flops = heads * 12 * tokens * tokens * width
    return pl.pallas_call(
        functools.partial(attention_kernel, step),
        grid=(heads,),
        out_shape=[jax.ShapeDtypeStruct(queries.shape, jnp.bfloat16)] * 3,
        in_specs=[
            pl.BlockSpec(memory_space=pltpu.SMEM),
            pl.BlockSpec(layout.shape, lambda h: (0, 0)),
            head, head, head, head, whole, whole,
        ],
        out_specs=[head] * 3,
        scratch_shapes=[pltpu.VMEM((tokens, width), jnp.float32)] * 2,
        cost_estimate=pl.CostEstimate(
            flops=flops, bytes_accessed=heads * 16 * tokens * width, transcendentals=heads * tokens * tokens
        ),
    )(flip, layout, queries, keys, values, grads, cosine, sine)


def turn_tables(positions):
    cosine, sine = rope_tables(positions)
    cosine, sine = cosine[:, 0], sine[:, 0]
    half = HEAD_DIM // 2
    return cosine, jnp.concatenate([sine[:, :half], -sine[:, half:]], axis=1)


def swapped_body(
    fixed_point, incoming, norm_gain, query_weight, key_weight, value_weight, out_weight, layout
):
    local_rows, model_width = fixed_point.shape
    head_width = query_weight.shape[1]
    head_count = head_width // HEAD_DIM
    seq_tokens = local_rows * lax.axis_size("tensor")
    seq_length = seq_tokens * lax.axis_size("seq")
    contract_last = (((1,), (1,)), ((), ()))
    head_shape = (seq_tokens, head_count, HEAD_DIM)
    flip = lax.axis_index("tensor") * local_rows
    order = jnp.arange(seq_length, dtype=jnp.int32) ^ flip
    cosine, sine = turn_tables(order)
    own = order[:seq_tokens] + lax.axis_index("seq") * seq_tokens
    own_cosine, own_sine = rope_tables(own)

    def normalized(rows):
        point = rows.astype(jnp.float32)
        inverse = lax.rsqrt(jnp.mean(point * point, axis=1, keepdims=True) + EPS)
        return point * inverse, inverse

    scaled, inv_rms = normalized(fixed_point)
    all_points = jnp.concatenate(xor_gather(fixed_point), axis=0)
    all_scaled, _ = normalized(all_points)
    normed = (norm_gain * all_scaled).astype(jnp.bfloat16)

    def project(weight):
        return jnp.dot(normed, weight, preferred_element_type=jnp.float32).reshape(head_shape)

    queries = swap_to_heads(
        rotate(project(query_weight), own_cosine, own_sine).astype(jnp.bfloat16)
    )
    keys = swap_to_heads(rotate(project(key_weight), own_cosine, own_sine).astype(jnp.bfloat16))
    values = swap_to_heads(project(value_weight).astype(jnp.bfloat16))

    cotangent = incoming
    adjoint = incoming.astype(jnp.float32)
    gain_part = jnp.zeros((model_width,), jnp.float32)
    for term_index in range(ITERS):
        terms = jnp.concatenate(xor_gather(cotangent.astype(jnp.bfloat16)), axis=0)
        grad_out = lax.dot_general(
            terms, out_weight, contract_last, preferred_element_type=jnp.float32
        )
        grads = swap_to_heads(grad_out.astype(jnp.bfloat16).reshape(head_shape))
        grad_query, grad_key, grad_value = attention_grads(
            flip[None], seq_tokens, layout, queries, keys, values, grads, cosine, sine
        )
        total = lax.dot_general(
            swap_to_tokens(grad_value), value_weight, contract_last,
            preferred_element_type=jnp.float32,
        )
        total = total + lax.dot_general(
            swap_to_tokens(grad_key), key_weight, contract_last,
            preferred_element_type=jnp.float32,
        )
        total = total + lax.dot_general(
            swap_to_tokens(grad_query), query_weight, contract_last,
            preferred_element_type=jnp.float32,
        )
        gain_part = gain_part + jnp.sum(total * all_scaled, axis=0)
        grad_normed = xor_reduce_scatter(total)
        weighted = norm_gain * grad_normed
        inner = jnp.sum(weighted * scaled, axis=1, keepdims=True)
        cotangent = inv_rms * (weighted - scaled * (inner / model_width))
        adjoint = adjoint + cotangent
    return (adjoint, all_sum(gain_part) * seq_length ** (-0.5))


def power_of_two(number):
    return number & (number - 1) == 0


def solution(mesh):
    in_specs = (
        P(("seq", "tensor"), None),
        P(("seq", "tensor"), None),
        P(),
        P(None, "tensor"),
        P(None, "tensor"),
        P(None, "tensor"),
        P("tensor", None),
        P(),
    )
    out_specs = (P(("seq", "tensor"), None), P())
    seq, tensor = mesh.shape["seq"], mesh.shape["tensor"]

    def whole(*arguments):
        local_rows = arguments[0].shape[0] // (seq * tensor)
        heads = arguments[3].shape[1] // (HEAD_DIM * tensor)
        fits = (
            heads % seq == 0
            and all(map(power_of_two, (seq, tensor, local_rows)))
            and local_rows * tensor % BLK == 0
        )
        body = swapped_body if fits else gathered_body
        return jax.shard_map(
            body, mesh=mesh, in_specs=in_specs, out_specs=out_specs, check_vma=False
        )(*arguments)

    return whole
```

```python
import functools

import jax
import jax.numpy as jnp
from jax import lax
from jax.experimental import pallas as pl
from jax.experimental.pallas import tpu as pltpu
from jax.sharding import PartitionSpec as P

HEAD_DIM = 128
BLK = 64
ITERS = 2


EPS = 1e-05
THETA = 10000.0
MASKED = -1e30


def rope_tables(positions):
    freq = THETA ** (-jnp.arange(0, HEAD_DIM, 2, dtype=jnp.float32) / HEAD_DIM)
    angle = positions.astype(jnp.float32)[:, None] * freq[None, :]
    cosine = jnp.concatenate([jnp.cos(angle), jnp.cos(angle)], axis=1)[:, None, :]
    sine = jnp.concatenate([jnp.sin(angle), jnp.sin(angle)], axis=1)[:, None, :]
    return (cosine, sine)


def rotate(values, cosine, sine):
    half = HEAD_DIM // 2
    turned = jnp.concatenate([-values[..., half:], values[..., :half]], axis=-1)
    return values * cosine + turned * sine


def rotate_back(values, cosine, sine):
    half = HEAD_DIM // 2
    weighted = values * sine
    turned = jnp.concatenate([weighted[..., half:], -weighted[..., :half]], axis=-1)
    return values * cosine + turned


def expand_blocks(chosen):
    return jnp.repeat(jnp.repeat(chosen, BLK, axis=0), BLK, axis=1)


def pair_mask(query_pos, key_pos, chosen):
    query_block = (query_pos // BLK)[:, None]
    key_block = (key_pos // BLK)[None, :]
    earlier = (key_block < query_block) & chosen
    same = (key_block == query_block) & (key_pos[None, :] <= query_pos[:, None])
    return earlier | same


def gathered_body(
    fixed_point, incoming, norm_gain, query_weight, key_weight, value_weight, out_weight, layout
):
    local_rows, model_width = fixed_point.shape
    head_width = query_weight.shape[1]
    head_count = head_width // HEAD_DIM
    seq_tokens = local_rows * lax.axis_size("tensor")
    seq_length = seq_tokens * lax.axis_size("seq")
    seq_index = lax.axis_index("seq")
    score_scale = HEAD_DIM ** (-0.5)
    contract_last = (((1,), (1,)), ((), ()))
    head_shape = (seq_tokens, head_count, HEAD_DIM)
    point = fixed_point.astype(jnp.float32)
    inv_rms = lax.rsqrt(jnp.mean(point * point, axis=1, keepdims=True) + EPS)
    scaled = point * inv_rms
    normed = (norm_gain * scaled).astype(jnp.bfloat16)
    project_piece = lax.all_gather(normed, "tensor", axis=0, tiled=True)
    projected = jnp.concatenate(
        [
            jnp.dot(project_piece, query_weight, preferred_element_type=jnp.float32),
            jnp.dot(project_piece, key_weight, preferred_element_type=jnp.float32),
            jnp.dot(project_piece, value_weight, preferred_element_type=jnp.float32),
        ],
        axis=1,
    )
    positions = seq_index * seq_tokens + jnp.arange(seq_tokens, dtype=jnp.int32)
    cosine, sine = rope_tables(positions)
    queries = rotate(projected[:, :head_width].reshape(head_shape), cosine, sine).astype(
        jnp.bfloat16
    )
    keys = rotate(
        projected[:, head_width : 2 * head_width].reshape(head_shape), cosine, sine
    ).astype(jnp.bfloat16)
    values = projected[:, 2 * head_width :].reshape(head_shape).astype(jnp.bfloat16)
    block_rows = seq_tokens // BLK
    block_count = seq_length // BLK
    first_block = seq_index * block_rows
    key_positions = jnp.arange(seq_length, dtype=jnp.int32)
    chosen_rows = (
        lax.dynamic_slice(layout, (first_block, jnp.int32(0)), (block_rows, block_count)) > 0
    )
    allowed = pair_mask(positions, key_positions, expand_blocks(chosen_rows))
    keys_all, values_all = (
        lax.all_gather(keys, "seq", axis=0, tiled=True),
        lax.all_gather(values, "seq", axis=0, tiled=True),
    )
    scores = (
        jnp.einsum("qhd,khd->hqk", queries, keys_all, preferred_element_type=jnp.float32)
        * score_scale
    )
    scores = jnp.where(allowed[None], scores, MASKED)
    log_norm = jax.nn.logsumexp(scores, axis=2, keepdims=True)
    probs = jnp.exp(scores - log_norm)
    probs_low = probs.astype(jnp.bfloat16)
    attended = jnp.einsum(
        "hqk,khd->qhd", probs_low, values_all, preferred_element_type=jnp.float32
    ).astype(jnp.bfloat16)
    cotangent = incoming.astype(jnp.float32)
    adjoint = cotangent
    gain_grad = jnp.zeros((model_width,), jnp.float32)
    for term_index in range(ITERS):
        grad_out = lax.dot_general(
            lax.all_gather(cotangent.astype(jnp.bfloat16), "tensor", axis=0, tiled=True),
            out_weight,
            contract_last,
            preferred_element_type=jnp.float32,
        )
        grad_low = grad_out.astype(jnp.bfloat16).reshape(head_shape)
        delta = jnp.sum(grad_low.astype(jnp.float32) * attended.astype(jnp.float32), axis=2)
        grad_probs = jnp.einsum(
            "qhd,khd->hqk", grad_low, values_all, preferred_element_type=jnp.float32
        )
        grad_scores = (probs * (grad_probs - delta.T[:, :, None])).astype(jnp.bfloat16)
        grad_query = (
            jnp.einsum("hqk,khd->qhd", grad_scores, keys_all, preferred_element_type=jnp.float32)
            * score_scale
        )
        key_part = (
            jnp.einsum("hqk,qhd->khd", grad_scores, queries, preferred_element_type=jnp.float32)
            * score_scale
        )
        value_part = jnp.einsum(
            "hqk,qhd->khd", probs_low, grad_low, preferred_element_type=jnp.float32
        )
        key_grads = lax.psum_scatter(
            jnp.concatenate(
                [
                    key_part.reshape(seq_tokens * lax.axis_size("seq"), head_width),
                    value_part.reshape(seq_tokens * lax.axis_size("seq"), head_width),
                ],
                axis=1,
            ).astype(jnp.bfloat16),
            "seq",
            scatter_dimension=0,
            tiled=True,
        ).astype(jnp.float32)
        grad_key = key_grads[:, :head_width].reshape(head_shape)
        grad_value = key_grads[:, head_width:].reshape(head_shape)
        query_low = (
            rotate_back(grad_query, cosine, sine)
            .astype(jnp.bfloat16)
            .reshape(seq_tokens, head_width)
        )
        key_low = (
            rotate_back(grad_key, cosine, sine).astype(jnp.bfloat16).reshape(seq_tokens, head_width)
        )
        value_low = grad_value.astype(jnp.bfloat16).reshape(seq_tokens, head_width)
        total = lax.dot_general(
            query_low, query_weight, contract_last, preferred_element_type=jnp.float32
        )
        total = total + lax.dot_general(
            key_low, key_weight, contract_last, preferred_element_type=jnp.float32
        )
        total = total + lax.dot_general(
            value_low, value_weight, contract_last, preferred_element_type=jnp.float32
        )
        grad_normed = lax.psum_scatter(
            total.astype(jnp.bfloat16), "tensor", scatter_dimension=0, tiled=True
        ).astype(jnp.float32)
        gain_term = jnp.sum(grad_normed * scaled, axis=0)
        gain_grad = gain_grad + lax.psum(gain_term, ("seq", "tensor"))
        weighted = norm_gain * grad_normed
        inner = jnp.sum(weighted * scaled, axis=1, keepdims=True)
        cotangent = inv_rms * (weighted - scaled * (inner / model_width))
        adjoint = adjoint + cotangent
    return (adjoint, gain_grad * seq_length ** (-0.5))


def xor_pairs(axis, distance):
    return [(i, i ^ distance) for i in range(lax.axis_size(axis))]


def xor_gather(block):
    blocks = {0: block}
    distance = lax.axis_size("tensor") // 2
    while distance:
        blocks.update(
            {
                j ^ distance: lax.ppermute(b, "tensor", xor_pairs("tensor", distance))
                for j, b in list(blocks.items())
            }
        )
        distance //= 2
    return [blocks[j] for j in range(len(blocks))]


def xor_reduce_scatter(blocks):
    held = dict(enumerate(blocks))
    distance = 1
    while distance < lax.axis_size("tensor"):
        keep = [j for j in held if not j & distance]
        came = [
            lax.ppermute(
                held[j ^ distance].astype(jnp.bfloat16), "tensor", xor_pairs("tensor", distance)
            )
            for j in keep
        ]
        held = {
            j: held[j].astype(jnp.float32) + c.astype(jnp.float32) for j, c in zip(keep, came)
        }
        distance *= 2
    return held[0]


def all_sum(values):
    for axis in ("tensor", "seq"):
        distance = 1
        while distance < lax.axis_size(axis):
            values = values + lax.ppermute(values, axis, xor_pairs(axis, distance))
            distance *= 2
    return values


def swap(values):
    return lax.all_to_all(values, "seq", split_axis=0, concat_axis=0, tiled=True)


def contract(a, b, da, db):
    return lax.dot_general(
        a, b, (((da,), (db,)), ((), ())), preferred_element_type=jnp.float32
    )


def in_vmem(array):
    return pltpu.with_memory_space_constraint(array, pltpu.VMEM)


def vmem_specs(count):
    return [pl.BlockSpec(memory_space=pltpu.VMEM)] * count


def join_rows(refs, joined):
    rows = refs[0].shape[0]
    for i, ref in enumerate(refs):
        joined[i * rows : (i + 1) * rows, :] = ref[...]


def load_kernel(*refs, count, pieces):
    sources, targets, semaphores = refs[:count], refs[count : 2 * count], refs[-1]
    copies = []
    for i, (source, target) in enumerate(zip(sources, targets)):
        rows = source.shape[0] // pieces
        for j in range(pieces):
            part = pl.ds(j * rows, rows)
            copies.append(
                pltpu.make_async_copy(source.at[part], target.at[part], semaphores.at[i, j])
            )
    for copy in copies:
        copy.start()
    for copy in copies:
        copy.wait()


def load(weights, pieces=4):
    size = sum(w.size for w in weights)
    return pl.pallas_call(
        functools.partial(load_kernel, count=len(weights), pieces=pieces),
        out_shape=[pltpu.VMEM(w.shape, w.dtype) for w in weights],
        in_specs=[pl.BlockSpec(memory_space=pltpu.HBM)] * len(weights),
        out_specs=vmem_specs(len(weights)),
        scratch_shapes=[pltpu.SemaphoreType.DMA((len(weights), pieces))],
        compiler_params=pltpu.CompilerParams(vmem_limit_bytes=2**20),
        cost_estimate=pl.CostEstimate(
            flops=256 * size, bytes_accessed=2 * size, transcendentals=0
        ),
    )(*(pltpu.with_memory_space_constraint(w, pltpu.HBM) for w in weights))


def pull_back_kernel(*refs, pieces):
    terms, (weight_ref, out_ref, joined) = refs[:pieces], refs[pieces:]
    join_rows(terms, joined)
    dests, _, heads, _, width = out_ref.shape
    for index in range(dests * heads):
        grad = contract(joined[...], weight_ref[index * width : (index + 1) * width, :], 1, 1)
        out_ref[index // heads, 0, index % heads] = grad.astype(jnp.bfloat16)


def pull_back(terms, weight, seq):
    rows, model = terms[0].shape
    tokens = rows * len(terms)
    heads = weight.shape[0] // HEAD_DIM
    return pl.pallas_call(
        functools.partial(pull_back_kernel, pieces=len(terms)),
        out_shape=jax.ShapeDtypeStruct((seq, 1, heads // seq, tokens, HEAD_DIM), jnp.bfloat16),
        in_specs=vmem_specs(len(terms) + 1),
        out_specs=vmem_specs(1)[0],
        scratch_shapes=[pltpu.VMEM((tokens, model), jnp.bfloat16)],
        compiler_params=pltpu.CompilerParams(vmem_limit_bytes=8 * 2**20),
        cost_estimate=pl.CostEstimate(
            flops=2 * tokens * weight.size, bytes_accessed=2 * weight.size, transcendentals=0
        ),
    )(*terms, in_vmem(weight))


def project_kernel(*refs, pieces):
    points = refs[:pieces]
    gain_ref, cos_ref, sin_ref, *weights, out_ref, inverse_ref, normed = refs[pieces:]
    rows, model = points[0].shape
    for i, ref in enumerate(points):
        point = ref[...].astype(jnp.float32)
        inverse = lax.rsqrt(jnp.mean(point * point, axis=1, keepdims=True) + EPS)
        normed[i * rows : (i + 1) * rows, :] = (gain_ref[...] * (point * inverse)).astype(
            jnp.bfloat16
        )
        inverse_ref[i * rows : (i + 1) * rows, :] = jnp.broadcast_to(
            inverse, (rows, inverse_ref.shape[1])
        )
    dests, _, heads, _, width = out_ref.shape
    group = 2 if dests * heads % 2 == 0 else 1
    for which, weight in enumerate(weights):
        for first in range(0, dests * heads, group):
            wide = contract(
                normed[...], weight[:, first * width : (first + group) * width], 1, 0
            )
            for index in range(first, first + group):
                part = wide[:, (index - first) * width : (index - first + 1) * width]
                if which < 2:
                    part = part * cos_ref[...] - pltpu.roll(part, width // 2, 1) * sin_ref[...]
                out_ref[index // heads, which, index % heads] = part.astype(jnp.bfloat16)


def project(points, gain, cosine, sine, weights, seq):
    rows, model = points[0].shape
    tokens = rows * len(points)
    heads = weights[0].shape[1] // HEAD_DIM
    return pl.pallas_call(
        functools.partial(project_kernel, pieces=len(points)),
        out_shape=[
            jax.ShapeDtypeStruct((seq, 3, heads // seq, tokens, HEAD_DIM), jnp.bfloat16),
            jax.ShapeDtypeStruct((tokens, HEAD_DIM), jnp.float32),
        ],
        in_specs=vmem_specs(len(points) + 6),
        out_specs=vmem_specs(2),
        scratch_shapes=[pltpu.VMEM((tokens, model), jnp.bfloat16)],
        compiler_params=pltpu.CompilerParams(vmem_limit_bytes=12 * 2**20),
        cost_estimate=pl.CostEstimate(
            flops=6 * tokens * weights[0].size,
            bytes_accessed=6 * weights[0].size,
            transcendentals=0,
        ),
    )(*points, gain[None], cosine, sine, *map(in_vmem, weights))


def combine_kernel(*refs, pieces):
    points = refs[:pieces]
    inverse_ref, grads_ref, *weights = refs[pieces : pieces + 5]
    blocks = refs[pieces + 5 : 2 * pieces + 5]
    gain_ref, left = refs[2 * pieces + 5 :]
    rows, model = points[0].shape
    dests, _, heads, width, _ = grads_ref.shape
    for which in range(3):
        for index in range(dests * heads):
            left[which, :, index * width : (index + 1) * width] = grads_ref[
                index // heads, which, index % heads
            ].T
    step = min(512, model)
    for start in range(0, model, step):
        columns = slice(start, start + step)
        total = contract(left[0], weights[0][columns, :], 1, 1)
        for which in (1, 2):
            total = total + contract(left[which], weights[which][columns, :], 1, 1)
        low = total.astype(jnp.bfloat16)
        gain = jnp.zeros((1, step), jnp.float32)
        for i in range(pieces):
            part = low[i * rows : (i + 1) * rows, :]
            blocks[i][:, columns] = part
            scaled = points[i][:, columns].astype(jnp.float32) * inverse_ref[
                i * rows : (i + 1) * rows, :1
            ]
            gain = gain + jnp.sum(part.astype(jnp.float32) * scaled, axis=0, keepdims=True)
        gain_ref[:, columns] = gain


def combine(points, inverse, grads, weights):
    rows, model = points[0].shape
    tokens = rows * len(points)
    *outs, gain = pl.pallas_call(
        functools.partial(combine_kernel, pieces=len(points)),
        out_shape=[jax.ShapeDtypeStruct((rows, model), jnp.bfloat16)] * len(points)
        + [jax.ShapeDtypeStruct((1, model), jnp.float32)],
        in_specs=vmem_specs(len(points) + 5),
        out_specs=vmem_specs(len(points) + 1),
        scratch_shapes=[pltpu.VMEM((3, tokens, weights[0].shape[1]), jnp.bfloat16)],
        compiler_params=pltpu.CompilerParams(vmem_limit_bytes=12 * 2**20),
        cost_estimate=pl.CostEstimate(
            flops=6 * tokens * weights[0].size,
            bytes_accessed=6 * weights[0].size,
            transcendentals=0,
        ),
    )(*points, inverse, grads, *map(in_vmem, weights))
    return outs, gain[0]


def attention_kernel(
    flip_ref, layout_ref, qkv_ref, g_ref, cos_ref, sin_ref, out_ref, key_acc, value_acc, *, step
):
    size, _, _, rows, width = g_ref.shape
    tokens = size * rows
    blocks = layout_ref.shape[0]
    flip = flip_ref[0]
    scale = width ** (-0.5)
    half = width // 2

    def turn_back(grad, start, stop):
        turned = jnp.concatenate([grad[half:], -grad[:half]], axis=0)
        cosine = jnp.concatenate([cos_ref[:, start:stop]] * 2, axis=0)
        sine = jnp.concatenate([sin_ref[:, start:stop]] * 2, axis=0)
        return (grad * cosine + turned * sine).astype(jnp.bfloat16)

    def write(which, start, stop, value):
        for block in range(start // rows, stop // rows):
            out_ref[block, which, 0] = value[:, block * rows - start : (block + 1) * rows - start]

    queries, keys, values = (qkv_ref[:, i, 0].reshape(tokens, width) for i in range(3))
    grads = g_ref[:, 0, 0].reshape(tokens, width)
    key_t, value_t = keys.T, values.T
    layout = layout_ref[...].astype(jnp.float32).astype(jnp.bfloat16)
    key_acc[...] = jnp.zeros_like(key_acc)
    value_acc[...] = jnp.zeros_like(value_acc)
    for start in range(0, tokens, step):
        seen = start + step
        query = queries[start:seen]
        grad = grads[start:seen]
        key_pos = lax.broadcasted_iota(jnp.int32, (seen, step), 0) ^ flip
        query_pos = (lax.broadcasted_iota(jnp.int32, (seen, step), 1) + start) ^ flip
        key_hot = (
            lax.broadcasted_iota(jnp.int32, (seen, blocks), 1)
            == (lax.broadcasted_iota(jnp.int32, (seen, blocks), 0) ^ flip) // BLK
        )
        query_hot = (
            lax.broadcasted_iota(jnp.int32, (blocks, step), 0)
            == ((lax.broadcasted_iota(jnp.int32, (blocks, step), 1) + start) ^ flip) // BLK
        )
        key_rows = contract(
            key_hot.astype(jnp.float32).astype(jnp.bfloat16), layout, 1, 1
        ).astype(jnp.bfloat16)
        chosen = contract(
            key_rows, query_hot.astype(jnp.float32).astype(jnp.bfloat16), 1, 0
        )
        key_block, query_block = key_pos // BLK, query_pos // BLK
        allowed = ((key_block < query_block) & (chosen > 0.5)) | (
            (key_block == query_block) & (key_pos <= query_pos)
        )
        scores = contract(keys[:seen], query, 1, 1) * scale
        scores = jnp.where(allowed, scores, MASKED)
        probs = jnp.exp(scores - jnp.max(scores, axis=0, keepdims=True))
        probs = probs / jnp.sum(probs, axis=0, keepdims=True)
        low = probs.astype(jnp.bfloat16)
        attended = contract(value_t[:, :seen], low, 1, 0).astype(jnp.bfloat16).astype(jnp.float32)
        delta = jnp.sum(attended * grad.astype(jnp.float32).T, axis=0, keepdims=True)
        grad_probs = contract(values[:seen], grad, 1, 1)
        grad_scores = (probs * (grad_probs - delta)).astype(jnp.bfloat16)
        value_acc[:seen, :] += contract(low, grad, 1, 0)
        key_acc[:seen, :] += contract(grad_scores, query, 1, 0)
        grad_query = contract(key_t[:, :seen], grad_scores, 1, 0) * scale
        write(0, start, seen, turn_back(grad_query, start, seen))
    write(1, 0, tokens, turn_back(key_acc[...].T * scale, 0, tokens))
    write(2, 0, tokens, value_acc[...].T.astype(jnp.bfloat16))


def attention_grads(flip, layout, qkv, grads, cosine, sine):
    last = grads.shape[1] - 1
    size, _, heads, rows, width = qkv.shape
    tokens = size * rows
    table = pl.BlockSpec(cosine.shape, lambda h: (0, 0))
    return pl.pallas_call(
        functools.partial(attention_kernel, step=min(max(256, rows), tokens)),
        grid=(heads,),
        out_shape=jax.ShapeDtypeStruct((size, 3, heads, width, rows), jnp.bfloat16),
        in_specs=[
            pl.BlockSpec(memory_space=pltpu.SMEM),
            pl.BlockSpec(layout.shape, lambda h: (0, 0)),
            pl.BlockSpec((size, 3, 1, rows, width), lambda h: (0, 0, h, 0, 0)),
            pl.BlockSpec((size, 1, 1, rows, width), lambda h: (0, last, h, 0, 0)),
            table,
            table,
        ],
        out_specs=pl.BlockSpec((size, 3, 1, width, rows), lambda h: (0, 0, h, 0, 0)),
        scratch_shapes=[pltpu.VMEM((tokens, width), jnp.float32)] * 2,
        compiler_params=pltpu.CompilerParams(vmem_limit_bytes=14 * 2**20),
        cost_estimate=pl.CostEstimate(
            flops=heads * 12 * tokens * tokens * width,
            bytes_accessed=heads * 16 * tokens * width,
            transcendentals=heads * tokens * tokens,
        ),
    )(flip, layout, qkv, grads, cosine, sine)


def turn_tables(positions):
    freq = THETA ** (-jnp.arange(0, HEAD_DIM, 2, dtype=jnp.float32) / HEAD_DIM)
    angle = freq[:, None] * positions.astype(jnp.float32)[None, :]
    return jnp.cos(angle), jnp.sin(angle)


def swapped_body(
    fixed_point, incoming, norm_gain, query_weight, key_weight, value_weight, out_weight, layout
):
    local_rows, model_width = fixed_point.shape
    seq = lax.axis_size("seq")
    seq_tokens = local_rows * lax.axis_size("tensor")
    seq_length = seq_tokens * seq
    flip = lax.axis_index("tensor") * local_rows
    first = lax.axis_index("seq") * seq_tokens
    *weights, flip, first = lax.optimization_barrier(
        (query_weight, key_weight, value_weight, out_weight, flip, first)
    )
    *weights, out_weight = load(weights)
    order = jnp.arange(seq_length, dtype=jnp.int32) ^ flip
    cosine, sine = turn_tables(order)
    own_cosine, own_sine = (t[:, 0] for t in rope_tables(order[:seq_tokens] + first))
    half = HEAD_DIM // 2
    own_sine = jnp.concatenate([own_sine[:, :half], -own_sine[:, half:]], axis=1)

    points = xor_gather(fixed_point)
    late_incoming, _ = lax.optimization_barrier((incoming, points[-2]))
    grad_pieces = xor_gather(late_incoming)
    sent, inverse = project(points, norm_gain, own_cosine, own_sine, weights, seq)
    sent_grads = pull_back(grad_pieces, out_weight, seq)
    sent = jnp.concatenate([sent, sent_grads], axis=1)
    sent, cosine, sine = lax.optimization_barrier((sent, cosine, sine))
    qkv = grads = swap(sent)

    inv_rms = inverse[:local_rows, :1]
    scaled = fixed_point.astype(jnp.float32) * inv_rms
    adjoint = incoming.astype(jnp.float32)
    gain_part = jnp.zeros((model_width,), jnp.float32)
    for term_index in range(ITERS):
        if term_index:
            terms = xor_gather(cotangent.astype(jnp.bfloat16))
            grads = swap(pull_back(terms, out_weight, seq))
        back = swap(attention_grads(flip[None], layout, qkv, grads, cosine, sine))
        blocks, gain_term = combine(points, inverse, back, weights)
        gain_part = gain_part + gain_term
        grad_normed = xor_reduce_scatter(blocks)
        weighted = norm_gain * grad_normed
        inner = jnp.sum(weighted * scaled, axis=1, keepdims=True)
        cotangent = inv_rms * (weighted - scaled * (inner / model_width))
        adjoint = adjoint + cotangent
    return (adjoint, all_sum(gain_part) * seq_length ** (-0.5))


def power_of_two(number):
    return number & (number - 1) == 0


def solution(mesh):
    in_specs = (
        P(("seq", "tensor"), None),
        P(("seq", "tensor"), None),
        P(),
        P(None, "tensor"),
        P(None, "tensor"),
        P(None, "tensor"),
        P("tensor", None),
        P(),
    )
    out_specs = (P(("seq", "tensor"), None), P())
    seq, tensor = mesh.shape["seq"], mesh.shape["tensor"]

    def whole(*arguments):
        local_rows = arguments[0].shape[0] // (seq * tensor)
        heads = arguments[3].shape[1] // (HEAD_DIM * tensor)
        fits = (
            heads % seq == 0
            and all(map(power_of_two, (seq, tensor, local_rows)))
            and local_rows * tensor % BLK == 0
        )
        body = swapped_body if fits else gathered_body
        return jax.shard_map(
            body, mesh=mesh, in_specs=in_specs, out_specs=out_specs, check_vma=False
        )(*arguments)

    return whole
```

```python
import functools

import jax
import jax.numpy as jnp
from jax import lax
from jax.experimental import pallas as pl
from jax.experimental.pallas import tpu as pltpu
from jax.sharding import PartitionSpec as P


HEAD_DIM = 128
BLK = 64
ITERS = 2


EPS = 1e-05
THETA = 10000.0
MASKED = -1e30


def rope_tables(positions):
    freq = THETA ** (-jnp.arange(0, HEAD_DIM, 2, dtype=jnp.float32) / HEAD_DIM)
    angle = positions.astype(jnp.float32)[:, None] * freq[None, :]
    cosine = jnp.concatenate([jnp.cos(angle), jnp.cos(angle)], axis=1)[:, None, :]
    sine = jnp.concatenate([jnp.sin(angle), jnp.sin(angle)], axis=1)[:, None, :]
    return (cosine, sine)


def rotate(values, cosine, sine):
    half = HEAD_DIM // 2
    turned = jnp.concatenate([-values[..., half:], values[..., :half]], axis=-1)
    return values * cosine + turned * sine


def rotate_back(values, cosine, sine):
    half = HEAD_DIM // 2
    weighted = values * sine
    turned = jnp.concatenate([weighted[..., half:], -weighted[..., :half]], axis=-1)
    return values * cosine + turned


def expand_blocks(chosen):
    return jnp.repeat(jnp.repeat(chosen, BLK, axis=0), BLK, axis=1)


def pair_mask(query_pos, key_pos, chosen):
    query_block = (query_pos // BLK)[:, None]
    key_block = (key_pos // BLK)[None, :]
    earlier = (key_block < query_block) & chosen
    same = (key_block == query_block) & (key_pos[None, :] <= query_pos[:, None])
    return earlier | same


def gathered_body(
    fixed_point, incoming, norm_gain, query_weight, key_weight, value_weight, out_weight, layout
):
    local_rows, model_width = fixed_point.shape
    head_width = query_weight.shape[1]
    head_count = head_width // HEAD_DIM
    seq_tokens = local_rows * lax.axis_size("tensor")
    seq_length = seq_tokens * lax.axis_size("seq")
    seq_index = lax.axis_index("seq")
    score_scale = HEAD_DIM ** (-0.5)
    contract_last = (((1,), (1,)), ((), ()))
    head_shape = (seq_tokens, head_count, HEAD_DIM)
    point = fixed_point.astype(jnp.float32)
    inv_rms = lax.rsqrt(jnp.mean(point * point, axis=1, keepdims=True) + EPS)
    scaled = point * inv_rms
    normed = (norm_gain * scaled).astype(jnp.bfloat16)
    project_piece = lax.all_gather(normed, "tensor", axis=0, tiled=True)
    projected = jnp.concatenate(
        [
            jnp.dot(project_piece, query_weight, preferred_element_type=jnp.float32),
            jnp.dot(project_piece, key_weight, preferred_element_type=jnp.float32),
            jnp.dot(project_piece, value_weight, preferred_element_type=jnp.float32),
        ],
        axis=1,
    )
    positions = seq_index * seq_tokens + jnp.arange(seq_tokens, dtype=jnp.int32)
    cosine, sine = rope_tables(positions)
    queries = rotate(projected[:, :head_width].reshape(head_shape), cosine, sine).astype(
        jnp.bfloat16
    )
    keys = rotate(
        projected[:, head_width : 2 * head_width].reshape(head_shape), cosine, sine
    ).astype(jnp.bfloat16)
    values = projected[:, 2 * head_width :].reshape(head_shape).astype(jnp.bfloat16)
    block_rows = seq_tokens // BLK
    block_count = seq_length // BLK
    first_block = seq_index * block_rows
    key_positions = jnp.arange(seq_length, dtype=jnp.int32)
    chosen_rows = (
        lax.dynamic_slice(layout, (first_block, jnp.int32(0)), (block_rows, block_count)) > 0
    )
    allowed = pair_mask(positions, key_positions, expand_blocks(chosen_rows))
    keys_all, values_all = (
        lax.all_gather(keys, "seq", axis=0, tiled=True),
        lax.all_gather(values, "seq", axis=0, tiled=True),
    )
    scores = (
        jnp.einsum("qhd,khd->hqk", queries, keys_all, preferred_element_type=jnp.float32)
        * score_scale
    )
    scores = jnp.where(allowed[None], scores, MASKED)
    log_norm = jax.nn.logsumexp(scores, axis=2, keepdims=True)
    probs = jnp.exp(scores - log_norm)
    probs_low = probs.astype(jnp.bfloat16)
    attended = jnp.einsum(
        "hqk,khd->qhd", probs_low, values_all, preferred_element_type=jnp.float32
    ).astype(jnp.bfloat16)
    cotangent = incoming.astype(jnp.float32)
    adjoint = cotangent
    gain_grad = jnp.zeros((model_width,), jnp.float32)
    for _ in range(ITERS):
        grad_out = lax.dot_general(
            lax.all_gather(cotangent.astype(jnp.bfloat16), "tensor", axis=0, tiled=True),
            out_weight,
            contract_last,
            preferred_element_type=jnp.float32,
        )
        grad_low = grad_out.astype(jnp.bfloat16).reshape(head_shape)
        delta = jnp.sum(grad_low.astype(jnp.float32) * attended.astype(jnp.float32), axis=2)
        grad_probs = jnp.einsum(
            "qhd,khd->hqk", grad_low, values_all, preferred_element_type=jnp.float32
        )
        grad_scores = (probs * (grad_probs - delta.T[:, :, None])).astype(jnp.bfloat16)
        grad_query = (
            jnp.einsum("hqk,khd->qhd", grad_scores, keys_all, preferred_element_type=jnp.float32)
            * score_scale
        )
        key_part = (
            jnp.einsum("hqk,qhd->khd", grad_scores, queries, preferred_element_type=jnp.float32)
            * score_scale
        )
        value_part = jnp.einsum(
            "hqk,qhd->khd", probs_low, grad_low, preferred_element_type=jnp.float32
        )
        key_grads = lax.psum_scatter(
            jnp.concatenate(
                [
                    key_part.reshape(seq_tokens * lax.axis_size("seq"), head_width),
                    value_part.reshape(seq_tokens * lax.axis_size("seq"), head_width),
                ],
                axis=1,
            ).astype(jnp.bfloat16),
            "seq",
            scatter_dimension=0,
            tiled=True,
        ).astype(jnp.float32)
        grad_key = key_grads[:, :head_width].reshape(head_shape)
        grad_value = key_grads[:, head_width:].reshape(head_shape)
        query_low = (
            rotate_back(grad_query, cosine, sine)
            .astype(jnp.bfloat16)
            .reshape(seq_tokens, head_width)
        )
        key_low = (
            rotate_back(grad_key, cosine, sine).astype(jnp.bfloat16).reshape(seq_tokens, head_width)
        )
        value_low = grad_value.astype(jnp.bfloat16).reshape(seq_tokens, head_width)
        total = lax.dot_general(
            query_low, query_weight, contract_last, preferred_element_type=jnp.float32
        )
        total = total + lax.dot_general(
            key_low, key_weight, contract_last, preferred_element_type=jnp.float32
        )
        total = total + lax.dot_general(
            value_low, value_weight, contract_last, preferred_element_type=jnp.float32
        )
        grad_normed = lax.psum_scatter(
            total.astype(jnp.bfloat16), "tensor", scatter_dimension=0, tiled=True
        ).astype(jnp.float32)
        gain_term = jnp.sum(grad_normed * scaled, axis=0)
        gain_grad = gain_grad + lax.psum(gain_term, ("seq", "tensor"))
        weighted = norm_gain * grad_normed
        inner = jnp.sum(weighted * scaled, axis=1, keepdims=True)
        cotangent = inv_rms * (weighted - scaled * (inner / model_width))
        adjoint = adjoint + cotangent
    return (adjoint, gain_grad * seq_length ** (-0.5))


def xor_pairs(axis, distance):
    return [(i, i ^ distance) for i in range(lax.axis_size(axis))]


def xor_gather(block):
    blocks = {0: block}
    distance = lax.axis_size("tensor") // 2
    while distance:
        blocks.update(
            {
                j ^ distance: lax.ppermute(b, "tensor", xor_pairs("tensor", distance))
                for j, b in list(blocks.items())
            }
        )
        distance //= 2
    return [blocks[j] for j in range(len(blocks))]


def xor_reduce_scatter(blocks):
    held = {j: [block] for j, block in enumerate(blocks)}
    distance = 1
    while distance < lax.axis_size("tensor"):
        for j in [j for j in held if not j & distance]:
            parts = held.pop(j ^ distance)
            if len(parts) > 1:
                parts = [sum(p.astype(jnp.float32) for p in parts).astype(jnp.bfloat16)]
            held[j].append(lax.ppermute(parts[0], "tensor", xor_pairs("tensor", distance)))
        distance *= 2
    return held[0]


def all_sum(values):
    axes = ("seq", "tensor")
    size = lax.axis_size("seq") * lax.axis_size("tensor")
    bits = [1 << i for i in range(size.bit_length() - 1)]
    phases = [bits[:1]] + [bits[i : i + 2] for i in range(1, len(bits), 2)][::-1]
    for phase in phases:
        parts = [values]
        for flips in range(1, 1 << len(phase)):
            distance = sum(bit for i, bit in enumerate(phase) if flips >> i & 1)
            parts.append(lax.ppermute(values, axes, [(i, i ^ distance) for i in range(size)]))
        while len(parts) > 1:
            parts = [x + y for x, y in zip(parts[::2], parts[1::2])]
        values = parts[0]
    return values


def swap(values):
    return lax.all_to_all(values, "seq", split_axis=0, concat_axis=0, tiled=True)


def contract(a, b, da, db):
    return lax.dot_general(
        a, b, (((da,), (db,)), ((), ())), preferred_element_type=jnp.float32
    )


def in_vmem(array):
    return pltpu.with_memory_space_constraint(array, pltpu.VMEM)


def vmem_specs(count):
    return [pl.BlockSpec(memory_space=pltpu.VMEM)] * count


def join_rows(refs, joined):
    rows = refs[0].shape[0]
    for i, ref in enumerate(refs):
        joined[i * rows : (i + 1) * rows, :] = ref[...]


def load_kernel(*refs, count, pieces):
    sources, targets, semaphores = refs[:count], refs[count : 2 * count], refs[-1]
    copies = []
    for i, (source, target) in enumerate(zip(sources, targets)):
        rows = source.shape[0] // pieces
        for j in range(pieces):
            part = pl.ds(j * rows, rows)
            copies.append(
                pltpu.make_async_copy(source.at[part], target.at[part], semaphores.at[i, j])
            )
    for copy in copies:
        copy.start()
    for copy in copies:
        copy.wait()


def load(weights, pieces=4):
    size = sum(w.size for w in weights)
    return pl.pallas_call(
        functools.partial(load_kernel, count=len(weights), pieces=pieces),
        out_shape=[pltpu.VMEM(w.shape, w.dtype) for w in weights],
        in_specs=[pl.BlockSpec(memory_space=pltpu.HBM)] * len(weights),
        out_specs=vmem_specs(len(weights)),
        scratch_shapes=[pltpu.SemaphoreType.DMA((len(weights), pieces))],
        compiler_params=pltpu.CompilerParams(vmem_limit_bytes=2**20),
        cost_estimate=pl.CostEstimate(
            flops=256 * size, bytes_accessed=2 * size, transcendentals=0
        ),
    )(*(pltpu.with_memory_space_constraint(w, pltpu.HBM) for w in weights))


def pull_back_kernel(*refs, pieces):
    terms, (weight_ref, out_ref, joined) = refs[:pieces], refs[pieces:]
    join_rows(terms, joined)
    dests, _, heads, _, width = out_ref.shape
    for index in range(dests * heads):
        grad = contract(joined[...], weight_ref[index * width : (index + 1) * width, :], 1, 1)
        out_ref[index // heads, 0, index % heads] = grad.astype(jnp.bfloat16)


def pull_back(terms, weight, seq):
    rows, model = terms[0].shape
    tokens = rows * len(terms)
    heads = weight.shape[0] // HEAD_DIM
    return pl.pallas_call(
        functools.partial(pull_back_kernel, pieces=len(terms)),
        out_shape=jax.ShapeDtypeStruct((seq, 1, heads // seq, tokens, HEAD_DIM), jnp.bfloat16),
        in_specs=vmem_specs(len(terms) + 1),
        out_specs=vmem_specs(1)[0],
        scratch_shapes=[pltpu.VMEM((tokens, model), jnp.bfloat16)],
        compiler_params=pltpu.CompilerParams(vmem_limit_bytes=8 * 2**20),
        cost_estimate=pl.CostEstimate(
            flops=2 * tokens * weight.size, bytes_accessed=2 * weight.size, transcendentals=0
        ),
    )(*terms, in_vmem(weight))


def project_kernel(*refs, pieces):
    points = refs[:pieces]
    gain_ref, cos_ref, sin_ref, *weights, out_ref, inverse_ref, normed = refs[pieces:]
    rows, _ = points[0].shape
    for i, ref in enumerate(points):
        point = ref[...].astype(jnp.float32)
        inverse = lax.rsqrt(jnp.mean(point * point, axis=1, keepdims=True) + EPS)
        normed[i * rows : (i + 1) * rows, :] = (gain_ref[...] * (point * inverse)).astype(
            jnp.bfloat16
        )
        inverse_ref[i * rows : (i + 1) * rows, :] = jnp.broadcast_to(
            inverse, (rows, inverse_ref.shape[1])
        )
    dests, _, heads, _, width = out_ref.shape
    group = 2 if dests * heads % 2 == 0 else 1
    for which, weight in enumerate(weights):
        for first in range(0, dests * heads, group):
            wide = contract(
                normed[...], weight[:, first * width : (first + group) * width], 1, 0
            )
            for index in range(first, first + group):
                part = wide[:, (index - first) * width : (index - first + 1) * width]
                if which < 2:
                    part = part * cos_ref[...] - pltpu.roll(part, width // 2, 1) * sin_ref[...]
                out_ref[index // heads, which, index % heads] = part.astype(jnp.bfloat16)


def project(points, gain, cosine, sine, weights, seq):
    rows, model = points[0].shape
    tokens = rows * len(points)
    heads = weights[0].shape[1] // HEAD_DIM
    return pl.pallas_call(
        functools.partial(project_kernel, pieces=len(points)),
        out_shape=[
            jax.ShapeDtypeStruct((seq, 3, heads // seq, tokens, HEAD_DIM), jnp.bfloat16),
            jax.ShapeDtypeStruct((tokens, HEAD_DIM), jnp.float32),
        ],
        in_specs=vmem_specs(len(points) + 6),
        out_specs=vmem_specs(2),
        scratch_shapes=[pltpu.VMEM((tokens, model), jnp.bfloat16)],
        compiler_params=pltpu.CompilerParams(vmem_limit_bytes=12 * 2**20),
        cost_estimate=pl.CostEstimate(
            flops=6 * tokens * weights[0].size,
            bytes_accessed=6 * weights[0].size,
            transcendentals=0,
        ),
    )(*points, gain[None], cosine, sine, *map(in_vmem, weights))


def combine_kernel(*refs, pieces, columns, turned):
    points, (inverse_ref, grads_ref, *weights), refs = (
        refs[:pieces], refs[pieces : pieces + 5], refs[pieces + 5 :]
    )
    blocks, gain_ref = refs[:pieces], refs[pieces]
    rows = points[0].shape[0]
    if turned:
        left = grads_ref
    else:
        left = refs[pieces + 1]
        dests, _, heads, width, _ = grads_ref.shape
        for which in range(3):
            for index in range(dests * heads):
                left[which, :, index * width : (index + 1) * width] = grads_ref[
                    index // heads, which, index % heads
                ].T
    first, last = columns
    step = min(512, last - first)
    for start in range(first, last, step):
        source = slice(start, start + step)
        target = slice(start - first, start - first + step)
        total = contract(left[0], weights[0][source, :], 1, 1)
        for which in (1, 2):
            total = total + contract(left[which], weights[which][source, :], 1, 1)
        low = total.astype(jnp.bfloat16)
        gain = jnp.zeros((1, step), jnp.float32)
        for i in range(pieces):
            part = low[i * rows : (i + 1) * rows, :]
            blocks[i][:, target] = part
            scaled = points[i][:, source].astype(jnp.float32) * inverse_ref[
                i * rows : (i + 1) * rows, :1
            ]
            gain = gain + jnp.sum(part.astype(jnp.float32) * scaled, axis=0, keepdims=True)
        gain_ref[:, target] = gain


def combine(points, inverse, grads, weights, columns):
    rows = points[0].shape[0]
    tokens, width = rows * len(points), columns[1] - columns[0]
    turned = grads.ndim == 3
    joined = (3, tokens, weights[0].shape[1])
    outs = pl.pallas_call(
        functools.partial(combine_kernel, pieces=len(points), columns=columns, turned=turned),
        out_shape=[jax.ShapeDtypeStruct((rows, width), jnp.bfloat16)] * len(points)
        + [jax.ShapeDtypeStruct((1, width), jnp.float32)]
        + [pltpu.VMEM(joined, jnp.bfloat16)] * (not turned),
        in_specs=vmem_specs(len(points) + 5),
        out_specs=vmem_specs(len(points) + 2 - turned),
        compiler_params=pltpu.CompilerParams(vmem_limit_bytes=8 * 2**20),
        cost_estimate=pl.CostEstimate(
            flops=6 * tokens * width * weights[0].shape[1],
            bytes_accessed=6 * width * weights[0].shape[1],
            transcendentals=0,
        ),
    )(*points, inverse, in_vmem(grads) if turned else grads, *map(in_vmem, weights))
    count = len(points)
    return outs[:count], outs[count][0], grads if turned else outs[count + 1]


def advance_kernel(*refs, parts):
    sums, (point_ref, inverse_ref, gain_ref, past_ref, next_ref, total_ref) = (
        refs[: sum(parts)], refs[sum(parts) :]
    )
    rows, model = point_ref.shape
    inverse = inverse_ref[:rows, :1]
    grads, first = [], 0
    for count in parts:
        group = sums[first : first + count]
        grads.append(sum(ref[...].astype(jnp.float32) for ref in group))
        first += count
    edges = [0]
    for grad in grads:
        edges.append(edges[-1] + grad.shape[1])
    spans = [slice(*edge) for edge in zip(edges, edges[1:])]
    scaled = [point_ref[:, s].astype(jnp.float32) * inverse for s in spans]
    weighted = [gain_ref[:, s] * g for s, g in zip(spans, grads)]
    inner = sum(jnp.sum(w * x, axis=1, keepdims=True) for w, x in zip(weighted, scaled))
    for s, w, x in zip(spans, weighted, scaled):
        term = inverse * (w - x * (inner / model))
        next_ref[:, s] = term.astype(jnp.bfloat16)
        total_ref[:, s] = past_ref[:, s].astype(jnp.float32) + term


def advance(sums, point, inverse, gain, past):
    return pl.pallas_call(
        functools.partial(advance_kernel, parts=[len(group) for group in sums]),
        out_shape=[
            jax.ShapeDtypeStruct(point.shape, jnp.bfloat16),
            jax.ShapeDtypeStruct(point.shape, jnp.float32),
        ],
        in_specs=vmem_specs(sum(map(len, sums)) + 4),
        out_specs=vmem_specs(2),
        compiler_params=pltpu.CompilerParams(vmem_limit_bytes=8 * 2**20),
        cost_estimate=pl.CostEstimate(
            flops=16 * point.size, bytes_accessed=16 * point.size, transcendentals=0
        ),
    )(*(p for group in sums for p in group), point, inverse, gain[None], past)


def attention_kernel(
    flip_ref, layout_ref, qkv_ref, g_ref, cos_ref, sin_ref, *refs, step, kept
):
    if kept:
        probs_ref, attended_ref, out_ref, key_acc, value_acc = refs
    else:
        out_ref, probs_ref, attended_ref, key_acc, value_acc = refs
    size, _, heads, rows, width = qkv_ref.shape
    last = g_ref.shape[1] - 1
    tokens = size * rows
    blocks = layout_ref.shape[0]
    flip = flip_ref[0]
    scale = width ** (-0.5)
    half = width // 2

    def turn_back(grad, start, stop):
        turned = jnp.concatenate([grad[half:], -grad[:half]], axis=0)
        cosine = jnp.concatenate([cos_ref[:, start:stop]] * 2, axis=0)
        sine = jnp.concatenate([sin_ref[:, start:stop]] * 2, axis=0)
        return (grad * cosine + turned * sine).astype(jnp.bfloat16)

    def probabilities(keys, query, start, seen):
        key_pos = lax.broadcasted_iota(jnp.int32, (seen, step), 0) ^ flip
        query_pos = (lax.broadcasted_iota(jnp.int32, (seen, step), 1) + start) ^ flip
        key_hot = (
            lax.broadcasted_iota(jnp.int32, (seen, blocks), 1)
            == (lax.broadcasted_iota(jnp.int32, (seen, blocks), 0) ^ flip) // BLK
        )
        query_hot = (
            lax.broadcasted_iota(jnp.int32, (blocks, step), 0)
            == ((lax.broadcasted_iota(jnp.int32, (blocks, step), 1) + start) ^ flip) // BLK
        )
        layout = layout_ref[...].astype(jnp.float32).astype(jnp.bfloat16)
        key_rows = contract(
            key_hot.astype(jnp.float32).astype(jnp.bfloat16), layout, 1, 1
        ).astype(jnp.bfloat16)
        chosen = contract(
            key_rows, query_hot.astype(jnp.float32).astype(jnp.bfloat16), 1, 0
        )
        key_block, query_block = key_pos // BLK, query_pos // BLK
        allowed = ((key_block < query_block) & (chosen > 0.5)) | (
            (key_block == query_block) & (key_pos <= query_pos)
        )
        scores = contract(keys[:seen], query, 1, 1) * scale
        scores = jnp.where(allowed, scores, MASKED)
        probs = jnp.exp(scores - jnp.max(scores, axis=0, keepdims=True))
        return probs * (1.0 / jnp.sum(probs, axis=0, keepdims=True))

    for head in range(heads):
        queries, keys, values = (qkv_ref[:, i, head].reshape(tokens, width) for i in range(3))
        grads = g_ref[:, last, head].reshape(tokens, width)
        key_t = keys.T
        key_acc[...] = jnp.zeros_like(key_acc)
        value_acc[...] = jnp.zeros_like(value_acc)

        def write(which, start, stop, value):
            for block in range(start // rows, stop // rows):
                out_ref[block, which, head] = value[
                    :, block * rows - start : (block + 1) * rows - start
                ]

        for start in range(0, tokens, step):
            seen = start + step
            query, grad = queries[start:seen], grads[start:seen]
            if kept:
                probs = probs_ref[head, :seen, start:seen]
            else:
                probs = probabilities(keys, query, start, seen)
                probs_ref[head, :seen, start:seen] = probs
            low = probs.astype(jnp.bfloat16)
            if kept:
                attended = attended_ref[head, :, start:seen]
            else:
                attended = contract(values.T[:, :seen], low, 1, 0).astype(jnp.bfloat16)
                attended_ref[head, :, start:seen] = attended
            delta = jnp.sum(
                attended.astype(jnp.float32) * grad.astype(jnp.float32).T, axis=0, keepdims=True
            )
            grad_probs = contract(values[:seen], grad, 1, 1)
            grad_scores = (probs * (grad_probs - delta)).astype(jnp.bfloat16)
            value_acc[:seen, :] += contract(low, grad, 1, 0)
            key_acc[:seen, :] += contract(grad_scores, query, 1, 0)
            grad_query = contract(key_t[:, :seen], grad_scores, 1, 0) * scale
            write(0, start, seen, turn_back(grad_query, start, seen))
        write(1, 0, tokens, turn_back(key_acc[...].T * scale, 0, tokens))
        write(2, 0, tokens, value_acc[...].T.astype(jnp.bfloat16))


def attention_grads(flip, layout, qkv, grads, cosine, sine, kept=()):
    size, _, heads, rows, width = qkv.shape
    tokens = size * rows
    keep = [
        pltpu.VMEM((heads, tokens, tokens), jnp.float32),
        pltpu.VMEM((heads, width, tokens), jnp.bfloat16),
    ]
    out, *new = pl.pallas_call(
        functools.partial(
            attention_kernel, step=min(max(256, rows), tokens), kept=bool(kept)
        ),
        out_shape=[jax.ShapeDtypeStruct((size, 3, heads, width, rows), jnp.bfloat16)]
        + keep * (not kept),
        in_specs=[pl.BlockSpec(memory_space=pltpu.SMEM)] + vmem_specs(5 + len(kept)),
        out_specs=vmem_specs(1 if kept else 3),
        scratch_shapes=[pltpu.VMEM((tokens, width), jnp.float32)] * 2,
        compiler_params=pltpu.CompilerParams(vmem_limit_bytes=12 * 2**20),
        cost_estimate=pl.CostEstimate(
            flops=heads * 12 * tokens * tokens * width,
            bytes_accessed=heads * 16 * tokens * width,
            transcendentals=0 if kept else heads * tokens * tokens,
        ),
    )(flip, layout, qkv, grads, cosine, sine, *map(in_vmem, kept))
    return out, kept or tuple(new)


def turn_tables(positions):
    freq = THETA ** (-jnp.arange(0, HEAD_DIM, 2, dtype=jnp.float32) / HEAD_DIM)
    angle = freq[:, None] * positions.astype(jnp.float32)[None, :]
    return jnp.cos(angle), jnp.sin(angle)


def swapped_body(
    fixed_point, incoming, norm_gain, query_weight, key_weight, value_weight, out_weight, layout
):
    local_rows, model_width = fixed_point.shape
    seq = lax.axis_size("seq")
    seq_tokens = local_rows * lax.axis_size("tensor")
    seq_length = seq_tokens * seq
    flip = lax.axis_index("tensor") * local_rows
    first = lax.axis_index("seq") * seq_tokens
    *weights, flip, first = lax.optimization_barrier(
        (query_weight, key_weight, value_weight, out_weight, flip, first)
    )
    *weights, out_weight = load(weights)
    order = jnp.arange(seq_length, dtype=jnp.int32) ^ flip
    cosine, sine = turn_tables(order)
    own_cosine, own_sine = (t[:, 0] for t in rope_tables(order[:seq_tokens] + first))
    half = HEAD_DIM // 2
    own_sine = jnp.concatenate([own_sine[:, :half], -own_sine[:, half:]], axis=1)

    points, grad_pieces = xor_gather(fixed_point), xor_gather(incoming)
    sent, inverse = project(points, norm_gain, own_cosine, own_sine, weights, seq)
    sent = jnp.concatenate([sent, pull_back(grad_pieces, out_weight, seq)], axis=1)
    sent, cosine, sine = lax.optimization_barrier((sent, cosine, sine))
    qkv = grads = swap(sent)

    cotangent = adjoint = incoming
    middle = model_width // 2
    gain_part, kept = jnp.zeros((model_width,), jnp.float32), ()
    for term_index in range(ITERS):
        if term_index:
            grads = swap(pull_back(xor_gather(cotangent), out_weight, seq))
        back, kept = attention_grads(flip[None], layout, qkv, grads, cosine, sine, kept)
        left = swap(back)
        sums, gains = [], []
        for columns in ((0, middle), (middle, model_width)):
            blocks, gain_term, left = combine(points, inverse, left, weights, columns)
            sums.append(xor_reduce_scatter(blocks))
            gains.append(gain_term)
        gain_part = gain_part + jnp.concatenate(gains)
        cotangent, adjoint = advance(sums, fixed_point, inverse, norm_gain, adjoint)
    return (adjoint, all_sum(gain_part) * seq_length ** (-0.5))


def power_of_two(number):
    return number & (number - 1) == 0


def solution(mesh):
    in_specs = (
        P(("seq", "tensor"), None),
        P(("seq", "tensor"), None),
        P(),
        P(None, "tensor"),
        P(None, "tensor"),
        P(None, "tensor"),
        P("tensor", None),
        P(),
    )
    out_specs = (P(("seq", "tensor"), None), P())
    seq, tensor = mesh.shape["seq"], mesh.shape["tensor"]

    def whole(*arguments):
        local_rows = arguments[0].shape[0] // (seq * tensor)
        heads = arguments[3].shape[1] // (HEAD_DIM * tensor)
        fits = (
            heads % seq == 0
            and all(map(power_of_two, (seq, tensor, local_rows)))
            and local_rows * tensor % BLK == 0
        )
        body = swapped_body if fits else gathered_body
        return jax.shard_map(
            body, mesh=mesh, in_specs=in_specs, out_specs=out_specs, check_vma=False
        )(*arguments)

    return whole
```

```python
import functools

import jax
import jax.numpy as jnp
from jax import lax
from jax.experimental import pallas as pl
from jax.experimental.pallas import tpu as pltpu
from jax.sharding import PartitionSpec as P


HEAD_DIM = 128
BLK = 64
ITERS = 2


EPS = 1e-05
THETA = 10000.0
MASKED = -1e30


def rope_tables(positions):
    freq = THETA ** (-jnp.arange(0, HEAD_DIM, 2, dtype=jnp.float32) / HEAD_DIM)
    angle = positions.astype(jnp.float32)[:, None] * freq[None, :]
    cosine = jnp.concatenate([jnp.cos(angle), jnp.cos(angle)], axis=1)[:, None, :]
    sine = jnp.concatenate([jnp.sin(angle), jnp.sin(angle)], axis=1)[:, None, :]
    return (cosine, sine)


def rotate(values, cosine, sine):
    half = HEAD_DIM // 2
    turned = jnp.concatenate([-values[..., half:], values[..., :half]], axis=-1)
    return values * cosine + turned * sine


def rotate_back(values, cosine, sine):
    half = HEAD_DIM // 2
    weighted = values * sine
    turned = jnp.concatenate([weighted[..., half:], -weighted[..., :half]], axis=-1)
    return values * cosine + turned


def expand_blocks(chosen):
    return jnp.repeat(jnp.repeat(chosen, BLK, axis=0), BLK, axis=1)


def pair_mask(query_pos, key_pos, chosen):
    query_block = (query_pos // BLK)[:, None]
    key_block = (key_pos // BLK)[None, :]
    earlier = (key_block < query_block) & chosen
    same = (key_block == query_block) & (key_pos[None, :] <= query_pos[:, None])
    return earlier | same


def gathered_body(
    fixed_point, incoming, norm_gain, query_weight, key_weight, value_weight, out_weight, layout
):
    local_rows, model_width = fixed_point.shape
    head_width = query_weight.shape[1]
    head_count = head_width // HEAD_DIM
    seq_tokens = local_rows * lax.axis_size("tensor")
    seq_length = seq_tokens * lax.axis_size("seq")
    seq_index = lax.axis_index("seq")
    score_scale = HEAD_DIM ** (-0.5)
    contract_last = (((1,), (1,)), ((), ()))
    head_shape = (seq_tokens, head_count, HEAD_DIM)
    point = fixed_point.astype(jnp.float32)
    inv_rms = lax.rsqrt(jnp.mean(point * point, axis=1, keepdims=True) + EPS)
    scaled = point * inv_rms
    normed = (norm_gain * scaled).astype(jnp.bfloat16)
    project_piece = lax.all_gather(normed, "tensor", axis=0, tiled=True)
    projected = jnp.concatenate(
        [
            jnp.dot(project_piece, query_weight, preferred_element_type=jnp.float32),
            jnp.dot(project_piece, key_weight, preferred_element_type=jnp.float32),
            jnp.dot(project_piece, value_weight, preferred_element_type=jnp.float32),
        ],
        axis=1,
    )
    positions = seq_index * seq_tokens + jnp.arange(seq_tokens, dtype=jnp.int32)
    cosine, sine = rope_tables(positions)
    queries = rotate(projected[:, :head_width].reshape(head_shape), cosine, sine).astype(
        jnp.bfloat16
    )
    keys = rotate(
        projected[:, head_width : 2 * head_width].reshape(head_shape), cosine, sine
    ).astype(jnp.bfloat16)
    values = projected[:, 2 * head_width :].reshape(head_shape).astype(jnp.bfloat16)
    block_rows = seq_tokens // BLK
    block_count = seq_length // BLK
    first_block = seq_index * block_rows
    key_positions = jnp.arange(seq_length, dtype=jnp.int32)
    chosen_rows = (
        lax.dynamic_slice(layout, (first_block, jnp.int32(0)), (block_rows, block_count)) > 0
    )
    allowed = pair_mask(positions, key_positions, expand_blocks(chosen_rows))
    keys_all, values_all = (
        lax.all_gather(keys, "seq", axis=0, tiled=True),
        lax.all_gather(values, "seq", axis=0, tiled=True),
    )
    scores = (
        jnp.einsum("qhd,khd->hqk", queries, keys_all, preferred_element_type=jnp.float32)
        * score_scale
    )
    scores = jnp.where(allowed[None], scores, MASKED)
    log_norm = jax.nn.logsumexp(scores, axis=2, keepdims=True)
    probs = jnp.exp(scores - log_norm)
    probs_low = probs.astype(jnp.bfloat16)
    attended = jnp.einsum(
        "hqk,khd->qhd", probs_low, values_all, preferred_element_type=jnp.float32
    ).astype(jnp.bfloat16)
    cotangent = incoming.astype(jnp.float32)
    adjoint = cotangent
    gain_grad = jnp.zeros((model_width,), jnp.float32)
    for _ in range(ITERS):
        grad_out = lax.dot_general(
            lax.all_gather(cotangent.astype(jnp.bfloat16), "tensor", axis=0, tiled=True),
            out_weight,
            contract_last,
            preferred_element_type=jnp.float32,
        )
        grad_low = grad_out.astype(jnp.bfloat16).reshape(head_shape)
        delta = jnp.sum(grad_low.astype(jnp.float32) * attended.astype(jnp.float32), axis=2)
        grad_probs = jnp.einsum(
            "qhd,khd->hqk", grad_low, values_all, preferred_element_type=jnp.float32
        )
        grad_scores = (probs * (grad_probs - delta.T[:, :, None])).astype(jnp.bfloat16)
        grad_query = (
            jnp.einsum("hqk,khd->qhd", grad_scores, keys_all, preferred_element_type=jnp.float32)
            * score_scale
        )
        key_part = (
            jnp.einsum("hqk,qhd->khd", grad_scores, queries, preferred_element_type=jnp.float32)
            * score_scale
        )
        value_part = jnp.einsum(
            "hqk,qhd->khd", probs_low, grad_low, preferred_element_type=jnp.float32
        )
        key_grads = lax.psum_scatter(
            jnp.concatenate(
                [
                    key_part.reshape(seq_tokens * lax.axis_size("seq"), head_width),
                    value_part.reshape(seq_tokens * lax.axis_size("seq"), head_width),
                ],
                axis=1,
            ).astype(jnp.bfloat16),
            "seq",
            scatter_dimension=0,
            tiled=True,
        ).astype(jnp.float32)
        grad_key = key_grads[:, :head_width].reshape(head_shape)
        grad_value = key_grads[:, head_width:].reshape(head_shape)
        query_low = (
            rotate_back(grad_query, cosine, sine)
            .astype(jnp.bfloat16)
            .reshape(seq_tokens, head_width)
        )
        key_low = (
            rotate_back(grad_key, cosine, sine).astype(jnp.bfloat16).reshape(seq_tokens, head_width)
        )
        value_low = grad_value.astype(jnp.bfloat16).reshape(seq_tokens, head_width)
        total = lax.dot_general(
            query_low, query_weight, contract_last, preferred_element_type=jnp.float32
        )
        total = total + lax.dot_general(
            key_low, key_weight, contract_last, preferred_element_type=jnp.float32
        )
        total = total + lax.dot_general(
            value_low, value_weight, contract_last, preferred_element_type=jnp.float32
        )
        grad_normed = lax.psum_scatter(
            total.astype(jnp.bfloat16), "tensor", scatter_dimension=0, tiled=True
        ).astype(jnp.float32)
        gain_term = jnp.sum(grad_normed * scaled, axis=0)
        gain_grad = gain_grad + lax.psum(gain_term, ("seq", "tensor"))
        weighted = norm_gain * grad_normed
        inner = jnp.sum(weighted * scaled, axis=1, keepdims=True)
        cotangent = inv_rms * (weighted - scaled * (inner / model_width))
        adjoint = adjoint + cotangent
    return (adjoint, gain_grad * seq_length ** (-0.5))


def xor_pairs(axis, distance):
    return [(i, i ^ distance) for i in range(lax.axis_size(axis))]


def xor_gather(block):
    blocks = {0: block}
    distance = lax.axis_size("tensor") // 2
    while distance:
        blocks.update(
            {
                j ^ distance: lax.ppermute(b, "tensor", xor_pairs("tensor", distance))
                for j, b in list(blocks.items())
            }
        )
        distance //= 2
    return [blocks[j] for j in range(len(blocks))]


def xor_reduce_scatter(blocks):
    held = {j: [block] for j, block in enumerate(blocks)}
    distance = 1
    while distance < lax.axis_size("tensor"):
        for j in [j for j in held if not j & distance]:
            parts = held.pop(j ^ distance)
            if len(parts) > 1:
                parts = [sum(p.astype(jnp.float32) for p in parts).astype(jnp.bfloat16)]
            held[j].append(lax.ppermute(parts[0], "tensor", xor_pairs("tensor", distance)))
        distance *= 2
    return held[0]


def all_sum(values):
    axes = ("seq", "tensor")
    size = lax.axis_size("seq") * lax.axis_size("tensor")
    bits = [1 << i for i in range(size.bit_length() - 1)]
    phases = [bits[:1]] + [bits[i : i + 2] for i in range(1, len(bits), 2)][::-1]
    for phase in phases:
        parts = [values]
        for flips in range(1, 1 << len(phase)):
            distance = sum(bit for i, bit in enumerate(phase) if flips >> i & 1)
            parts.append(lax.ppermute(values, axes, [(i, i ^ distance) for i in range(size)]))
        while len(parts) > 1:
            parts = [x + y for x, y in zip(parts[::2], parts[1::2])]
        values = parts[0]
    return values


def swap(values):
    return lax.all_to_all(values, "seq", split_axis=0, concat_axis=0, tiled=True)


def contract(a, b, da, db):
    return lax.dot_general(
        a, b, (((da,), (db,)), ((), ())), preferred_element_type=jnp.float32
    )


def in_vmem(array):
    return pltpu.with_memory_space_constraint(array, pltpu.VMEM)


def vmem_specs(count):
    return [pl.BlockSpec(memory_space=pltpu.VMEM)] * count


def join_rows(refs, joined):
    rows = refs[0].shape[0]
    for i, ref in enumerate(refs):
        joined[i * rows : (i + 1) * rows, :] = ref[...]


PIECES = 4


def in_hbm(array):
    return pltpu.with_memory_space_constraint(array, pltpu.HBM)


def copies_of(source, target, semaphores):
    rows = source.shape[0] // PIECES
    return [
        pltpu.make_async_copy(
            source.at[pl.ds(j * rows, rows)], target.at[pl.ds(j * rows, rows)], semaphores.at[j]
        )
        for j in range(PIECES)
    ]


def load_kernel(*refs, count):
    copies = []
    for i in range(count):
        copies += copies_of(refs[i], refs[count + i], refs[-1].at[i])
    for copy in copies:
        copy.start()
    for copy in copies:
        copy.wait()


def load(weights):
    size = sum(w.size for w in weights)
    return pl.pallas_call(
        functools.partial(load_kernel, count=len(weights)),
        out_shape=[pltpu.VMEM(w.shape, w.dtype) for w in weights],
        in_specs=[pl.BlockSpec(memory_space=pltpu.HBM)] * len(weights),
        out_specs=vmem_specs(len(weights)),
        scratch_shapes=[pltpu.SemaphoreType.DMA((len(weights), PIECES))],
        compiler_params=pltpu.CompilerParams(vmem_limit_bytes=2**20),
        cost_estimate=pl.CostEstimate(
            flops=256 * size, bytes_accessed=2 * size, transcendentals=0
        ),
    )(*map(in_hbm, weights))


def pull_back_kernel(*refs, pieces):
    terms, (weight_ref, out_ref, joined) = refs[:pieces], refs[pieces:]
    join_rows(terms, joined)
    dests, _, heads, _, width = out_ref.shape
    for index in range(dests * heads):
        grad = contract(joined[...], weight_ref[index * width : (index + 1) * width, :], 1, 1)
        out_ref[index // heads, 0, index % heads] = grad.astype(jnp.bfloat16)


def pull_back(terms, weight, seq):
    rows, model = terms[0].shape
    tokens = rows * len(terms)
    heads = weight.shape[0] // HEAD_DIM
    return pl.pallas_call(
        functools.partial(pull_back_kernel, pieces=len(terms)),
        out_shape=jax.ShapeDtypeStruct((seq, 1, heads // seq, tokens, HEAD_DIM), jnp.bfloat16),
        in_specs=vmem_specs(len(terms) + 1),
        out_specs=vmem_specs(1)[0],
        scratch_shapes=[pltpu.VMEM((tokens, model), jnp.bfloat16)],
        compiler_params=pltpu.CompilerParams(vmem_limit_bytes=8 * 2**20),
        cost_estimate=pl.CostEstimate(
            flops=2 * tokens * weight.size, bytes_accessed=2 * weight.size, transcendentals=0
        ),
    )(*terms, in_vmem(weight))


def project_kernel(*refs, pieces):
    points = refs[:pieces]
    gain_ref, cos_ref, sin_ref, *weights, far_ref = refs[pieces : pieces + 6]
    out_ref, inverse_ref, last_ref, normed, semaphores = refs[pieces + 6 :]
    rows, _ = points[0].shape
    copies = copies_of(far_ref, last_ref, semaphores)
    for copy in copies:
        copy.start()
    for i, ref in enumerate(points):
        point = ref[...].astype(jnp.float32)
        inverse = lax.rsqrt(jnp.mean(point * point, axis=1, keepdims=True) + EPS)
        normed[i * rows : (i + 1) * rows, :] = (gain_ref[...] * (point * inverse)).astype(
            jnp.bfloat16
        )
        inverse_ref[i * rows : (i + 1) * rows, :] = jnp.broadcast_to(
            inverse, (rows, inverse_ref.shape[1])
        )
    dests, _, heads, _, width = out_ref.shape
    group = 2 if dests * heads % 2 == 0 else 1
    for which, weight in enumerate((*weights, last_ref)):
        if which == 2:
            for copy in copies:
                copy.wait()
        for first in range(0, dests * heads, group):
            wide = contract(
                normed[...], weight[:, first * width : (first + group) * width], 1, 0
            )
            for index in range(first, first + group):
                part = wide[:, (index - first) * width : (index - first + 1) * width]
                if which < 2:
                    part = part * cos_ref[...] - pltpu.roll(part, width // 2, 1) * sin_ref[...]
                out_ref[index // heads, which, index % heads] = part.astype(jnp.bfloat16)


def project(points, gain, cosine, sine, weights, seq):
    *weights, last = weights
    rows, model = points[0].shape
    tokens = rows * len(points)
    heads = weights[0].shape[1] // HEAD_DIM
    return pl.pallas_call(
        functools.partial(project_kernel, pieces=len(points)),
        out_shape=[
            jax.ShapeDtypeStruct((seq, 3, heads // seq, tokens, HEAD_DIM), jnp.bfloat16),
            jax.ShapeDtypeStruct((tokens, HEAD_DIM), jnp.float32),
            pltpu.VMEM(last.shape, last.dtype),
        ],
        in_specs=vmem_specs(len(points) + 5) + [pl.BlockSpec(memory_space=pltpu.HBM)],
        out_specs=vmem_specs(3),
        scratch_shapes=[
            pltpu.VMEM((tokens, model), jnp.bfloat16),
            pltpu.SemaphoreType.DMA((PIECES,)),
        ],
        compiler_params=pltpu.CompilerParams(vmem_limit_bytes=12 * 2**20),
        cost_estimate=pl.CostEstimate(
            flops=6 * tokens * weights[0].size,
            bytes_accessed=6 * weights[0].size,
            transcendentals=0,
        ),
    )(*points, gain[None], cosine, sine, *map(in_vmem, weights), in_hbm(last))


def combine_kernel(*refs, pieces, columns):
    points, (inverse_ref, grads_ref, *weights), refs = (
        refs[:pieces], refs[pieces : pieces + 5], refs[pieces + 5 :]
    )
    blocks, gain_ref = refs[:pieces], refs[pieces]
    rows = points[0].shape[0]
    dests, _, heads, width, tokens = grads_ref.shape
    first, last = columns
    step = min(512, last - first)
    for start in range(first, last, step):
        source = slice(start, start + step)
        target = slice(start - first, start - first + step)
        total = sum(
            contract(
                weights[which][source, :],
                grads_ref[:, which].reshape(dests * heads * width, tokens),
                1,
                0,
            )
            for which in range(3)
        )
        low = total.T.astype(jnp.bfloat16)
        gain = jnp.zeros((1, step), jnp.float32)
        for i in range(pieces):
            part = low[i * rows : (i + 1) * rows, :]
            blocks[i][:, target] = part
            scaled = points[i][:, source].astype(jnp.float32) * inverse_ref[
                i * rows : (i + 1) * rows, :1
            ]
            gain = gain + jnp.sum(part.astype(jnp.float32) * scaled, axis=0, keepdims=True)
        gain_ref[:, target] = gain


def combine(points, inverse, grads, weights, columns):
    rows = points[0].shape[0]
    tokens, width = rows * len(points), columns[1] - columns[0]
    *outs, gain = pl.pallas_call(
        functools.partial(combine_kernel, pieces=len(points), columns=columns),
        out_shape=[jax.ShapeDtypeStruct((rows, width), jnp.bfloat16)] * len(points)
        + [jax.ShapeDtypeStruct((1, width), jnp.float32)],
        in_specs=vmem_specs(len(points) + 5),
        out_specs=vmem_specs(len(points) + 1),
        compiler_params=pltpu.CompilerParams(vmem_limit_bytes=8 * 2**20),
        cost_estimate=pl.CostEstimate(
            flops=6 * tokens * width * weights[0].shape[1],
            bytes_accessed=6 * width * weights[0].shape[1],
            transcendentals=0,
        ),
    )(*points, inverse, in_vmem(grads), *map(in_vmem, weights))
    return outs, gain[0]


def advance_kernel(*refs, parts):
    sums, (point_ref, inverse_ref, gain_ref, past_ref, next_ref, total_ref) = (
        refs[: sum(parts)], refs[sum(parts) :]
    )
    rows, model = point_ref.shape
    inverse = inverse_ref[:rows, :1]
    grads, first = [], 0
    for count in parts:
        group = sums[first : first + count]
        grads.append(sum(ref[...].astype(jnp.float32) for ref in group))
        first += count
    edges = [0]
    for grad in grads:
        edges.append(edges[-1] + grad.shape[1])
    spans = [slice(*edge) for edge in zip(edges, edges[1:])]
    scaled = [point_ref[:, s].astype(jnp.float32) * inverse for s in spans]
    weighted = [gain_ref[:, s] * g for s, g in zip(spans, grads)]
    inner = sum(jnp.sum(w * x, axis=1, keepdims=True) for w, x in zip(weighted, scaled))
    for s, w, x in zip(spans, weighted, scaled):
        term = inverse * (w - x * (inner / model))
        next_ref[:, s] = term.astype(jnp.bfloat16)
        total_ref[:, s] = past_ref[:, s].astype(jnp.float32) + term


def advance(sums, point, inverse, gain, past):
    return pl.pallas_call(
        functools.partial(advance_kernel, parts=[len(group) for group in sums]),
        out_shape=[
            jax.ShapeDtypeStruct(point.shape, jnp.bfloat16),
            jax.ShapeDtypeStruct(point.shape, jnp.float32),
        ],
        in_specs=vmem_specs(sum(map(len, sums)) + 4),
        out_specs=vmem_specs(2),
        compiler_params=pltpu.CompilerParams(vmem_limit_bytes=8 * 2**20),
        cost_estimate=pl.CostEstimate(
            flops=16 * point.size, bytes_accessed=16 * point.size, transcendentals=0
        ),
    )(*(p for group in sums for p in group), point, inverse, gain[None], past)


def attention_kernel(
    flip_ref, layout_ref, qkv_ref, g_ref, cos_ref, sin_ref, *refs, step, kept
):
    if kept:
        probs_ref, attended_ref, out_ref, key_acc, value_acc = refs
    else:
        out_ref, probs_ref, attended_ref, key_acc, value_acc = refs
    size, _, heads, rows, width = qkv_ref.shape
    last = g_ref.shape[1] - 1
    tokens = size * rows
    blocks = layout_ref.shape[0]
    flip = flip_ref[0]
    scale = width ** (-0.5)
    half = width // 2

    def turn_back(grad, start, stop):
        turned = jnp.concatenate([grad[half:], -grad[:half]], axis=0)
        cosine = jnp.concatenate([cos_ref[:, start:stop]] * 2, axis=0)
        sine = jnp.concatenate([sin_ref[:, start:stop]] * 2, axis=0)
        return (grad * cosine + turned * sine).astype(jnp.bfloat16)

    def probabilities(keys, query, start, seen):
        key_pos = lax.broadcasted_iota(jnp.int32, (seen, step), 0) ^ flip
        query_pos = (lax.broadcasted_iota(jnp.int32, (seen, step), 1) + start) ^ flip
        key_hot = (
            lax.broadcasted_iota(jnp.int32, (seen, blocks), 1)
            == (lax.broadcasted_iota(jnp.int32, (seen, blocks), 0) ^ flip) // BLK
        )
        query_hot = (
            lax.broadcasted_iota(jnp.int32, (blocks, step), 0)
            == ((lax.broadcasted_iota(jnp.int32, (blocks, step), 1) + start) ^ flip) // BLK
        )
        layout = layout_ref[...].astype(jnp.float32).astype(jnp.bfloat16)
        key_rows = contract(
            key_hot.astype(jnp.float32).astype(jnp.bfloat16), layout, 1, 1
        ).astype(jnp.bfloat16)
        chosen = contract(
            key_rows, query_hot.astype(jnp.float32).astype(jnp.bfloat16), 1, 0
        )
        key_block, query_block = key_pos // BLK, query_pos // BLK
        allowed = ((key_block < query_block) & (chosen > 0.5)) | (
            (key_block == query_block) & (key_pos <= query_pos)
        )
        scores = contract(keys[:seen], query, 1, 1) * scale
        scores = jnp.where(allowed, scores, MASKED)
        probs = jnp.exp(scores - jnp.max(scores, axis=0, keepdims=True))
        return probs * (1.0 / jnp.sum(probs, axis=0, keepdims=True))

    for head in range(heads):
        queries, keys, values = (qkv_ref[:, i, head].reshape(tokens, width) for i in range(3))
        grads = g_ref[:, last, head].reshape(tokens, width)
        key_t = keys.T
        key_acc[...] = jnp.zeros_like(key_acc)
        value_acc[...] = jnp.zeros_like(value_acc)

        def write(which, start, stop, value):
            for block in range(start // rows, stop // rows):
                out_ref[block, which, head] = value[
                    :, block * rows - start : (block + 1) * rows - start
                ]

        for start in range(0, tokens, step):
            seen = start + step
            query, grad = queries[start:seen], grads[start:seen]
            if kept:
                probs = probs_ref[head, :seen, start:seen]
            else:
                probs = probabilities(keys, query, start, seen)
                probs_ref[head, :seen, start:seen] = probs
            low = probs.astype(jnp.bfloat16)
            if kept:
                attended = attended_ref[head, :, start:seen]
            else:
                attended = contract(values.T[:, :seen], low, 1, 0).astype(jnp.bfloat16)
                attended_ref[head, :, start:seen] = attended
            delta = jnp.sum(
                attended.astype(jnp.float32) * grad.astype(jnp.float32).T, axis=0, keepdims=True
            )
            grad_probs = contract(values[:seen], grad, 1, 1)
            grad_scores = (probs * (grad_probs - delta)).astype(jnp.bfloat16)
            value_acc[:seen, :] += contract(low, grad, 1, 0)
            key_acc[:seen, :] += contract(grad_scores, query, 1, 0)
            grad_query = contract(key_t[:, :seen], grad_scores, 1, 0) * scale
            write(0, start, seen, turn_back(grad_query, start, seen))
        write(1, 0, tokens, turn_back(key_acc[...].T * scale, 0, tokens))
        write(2, 0, tokens, value_acc[...].T.astype(jnp.bfloat16))


def attention_grads(flip, layout, qkv, grads, cosine, sine, kept=()):
    size, _, heads, rows, width = qkv.shape
    tokens = size * rows
    keep = [
        pltpu.VMEM((heads, tokens, tokens), jnp.float32),
        pltpu.VMEM((heads, width, tokens), jnp.bfloat16),
    ]
    out, *new = pl.pallas_call(
        functools.partial(
            attention_kernel, step=min(max(256, rows), tokens), kept=bool(kept)
        ),
        out_shape=[jax.ShapeDtypeStruct((size, 3, heads, width, rows), jnp.bfloat16)]
        + keep * (not kept),
        in_specs=[pl.BlockSpec(memory_space=pltpu.SMEM)] + vmem_specs(5 + len(kept)),
        out_specs=vmem_specs(1 if kept else 3),
        scratch_shapes=[pltpu.VMEM((tokens, width), jnp.float32)] * 2,
        compiler_params=pltpu.CompilerParams(vmem_limit_bytes=12 * 2**20),
        cost_estimate=pl.CostEstimate(
            flops=heads * 12 * tokens * tokens * width,
            bytes_accessed=heads * 16 * tokens * width,
            transcendentals=0 if kept else heads * tokens * tokens,
        ),
    )(flip, layout, qkv, grads, cosine, sine, *map(in_vmem, kept))
    return out, kept or tuple(new)


def turn_tables(positions):
    freq = THETA ** (-jnp.arange(0, HEAD_DIM, 2, dtype=jnp.float32) / HEAD_DIM)
    angle = freq[:, None] * positions.astype(jnp.float32)[None, :]
    return jnp.cos(angle), jnp.sin(angle)


def swapped_body(
    fixed_point, incoming, norm_gain, query_weight, key_weight, value_weight, out_weight, layout
):
    local_rows, model_width = fixed_point.shape
    seq = lax.axis_size("seq")
    seq_tokens = local_rows * lax.axis_size("tensor")
    seq_length = seq_tokens * seq
    flip = lax.axis_index("tensor") * local_rows
    first = lax.axis_index("seq") * seq_tokens
    *weights, flip, first = lax.optimization_barrier(
        (query_weight, key_weight, out_weight, flip, first)
    )
    *weights, out_weight = load(weights)
    order = jnp.arange(seq_length, dtype=jnp.int32) ^ flip
    cosine, sine = turn_tables(order)
    own_cosine, own_sine = (t[:, 0] for t in rope_tables(order[:seq_tokens] + first))
    half = HEAD_DIM // 2
    own_sine = jnp.concatenate([own_sine[:, :half], -own_sine[:, half:]], axis=1)

    points, grad_pieces = xor_gather(fixed_point), xor_gather(incoming)
    sent, inverse, value_weight = project(
        points, norm_gain, own_cosine, own_sine, (*weights, value_weight), seq
    )
    weights = (*weights, value_weight)
    sent = jnp.concatenate([sent, pull_back(grad_pieces, out_weight, seq)], axis=1)
    sent, cosine, sine = lax.optimization_barrier((sent, cosine, sine))
    qkv = grads = swap(sent)

    cotangent = adjoint = incoming
    middle = model_width // 2
    gain_part, kept = jnp.zeros((model_width,), jnp.float32), ()
    for term_index in range(ITERS):
        if term_index:
            grads = swap(pull_back(xor_gather(cotangent), out_weight, seq))
        back, kept = attention_grads(flip[None], layout, qkv, grads, cosine, sine, kept)
        left = swap(back)
        sums, gains = [], []
        for columns in ((0, middle), (middle, model_width)):
            blocks, gain_term = combine(points, inverse, left, weights, columns)
            sums.append(xor_reduce_scatter(blocks))
            gains.append(gain_term)
        gain_part = gain_part + jnp.concatenate(gains)
        cotangent, adjoint = advance(sums, fixed_point, inverse, norm_gain, adjoint)
    return (adjoint, all_sum(gain_part) * seq_length ** (-0.5))


def power_of_two(number):
    return number & (number - 1) == 0


def solution(mesh):
    in_specs = (
        P(("seq", "tensor"), None),
        P(("seq", "tensor"), None),
        P(),
        P(None, "tensor"),
        P(None, "tensor"),
        P(None, "tensor"),
        P("tensor", None),
        P(),
    )
    out_specs = (P(("seq", "tensor"), None), P())
    seq, tensor = mesh.shape["seq"], mesh.shape["tensor"]

    def whole(*arguments):
        local_rows = arguments[0].shape[0] // (seq * tensor)
        heads = arguments[3].shape[1] // (HEAD_DIM * tensor)
        fits = (
            heads % seq == 0
            and all(map(power_of_two, (seq, tensor, local_rows)))
            and local_rows * tensor % BLK == 0
        )
        body = swapped_body if fits else gathered_body
        return jax.shard_map(
            body, mesh=mesh, in_specs=in_specs, out_specs=out_specs, check_vma=False
        )(*arguments)

    return whole
```

```python
import functools

import jax
import jax.numpy as jnp
from jax import lax
from jax.experimental import pallas as pl
from jax.experimental.pallas import tpu as pltpu
from jax.sharding import PartitionSpec as P


HEAD_DIM = 128
BLK = 64
ITERS = 2


EPS = 1e-05
THETA = 10000.0
MASKED = -1e30


def rope_tables(positions):
    freq = THETA ** (-jnp.arange(0, HEAD_DIM, 2, dtype=jnp.float32) / HEAD_DIM)
    angle = positions.astype(jnp.float32)[:, None] * freq[None, :]
    cosine = jnp.concatenate([jnp.cos(angle), jnp.cos(angle)], axis=1)[:, None, :]
    sine = jnp.concatenate([jnp.sin(angle), jnp.sin(angle)], axis=1)[:, None, :]
    return (cosine, sine)


def rotate(values, cosine, sine):
    half = HEAD_DIM // 2
    turned = jnp.concatenate([-values[..., half:], values[..., :half]], axis=-1)
    return values * cosine + turned * sine


def rotate_back(values, cosine, sine):
    half = HEAD_DIM // 2
    weighted = values * sine
    turned = jnp.concatenate([weighted[..., half:], -weighted[..., :half]], axis=-1)
    return values * cosine + turned


def expand_blocks(chosen):
    return jnp.repeat(jnp.repeat(chosen, BLK, axis=0), BLK, axis=1)


def pair_mask(query_pos, key_pos, chosen):
    query_block = (query_pos // BLK)[:, None]
    key_block = (key_pos // BLK)[None, :]
    earlier = (key_block < query_block) & chosen
    same = (key_block == query_block) & (key_pos[None, :] <= query_pos[:, None])
    return earlier | same


def gathered_body(
    fixed_point, incoming, norm_gain, query_weight, key_weight, value_weight, out_weight, layout
):
    local_rows, model_width = fixed_point.shape
    head_width = query_weight.shape[1]
    head_count = head_width // HEAD_DIM
    seq_tokens = local_rows * lax.axis_size("tensor")
    seq_length = seq_tokens * lax.axis_size("seq")
    seq_index = lax.axis_index("seq")
    score_scale = HEAD_DIM ** (-0.5)
    contract_last = (((1,), (1,)), ((), ()))
    head_shape = (seq_tokens, head_count, HEAD_DIM)
    point = fixed_point.astype(jnp.float32)
    inv_rms = lax.rsqrt(jnp.mean(point * point, axis=1, keepdims=True) + EPS)
    scaled = point * inv_rms
    normed = (norm_gain * scaled).astype(jnp.bfloat16)
    project_piece = lax.all_gather(normed, "tensor", axis=0, tiled=True)
    projected = jnp.concatenate(
        [
            jnp.dot(project_piece, query_weight, preferred_element_type=jnp.float32),
            jnp.dot(project_piece, key_weight, preferred_element_type=jnp.float32),
            jnp.dot(project_piece, value_weight, preferred_element_type=jnp.float32),
        ],
        axis=1,
    )
    positions = seq_index * seq_tokens + jnp.arange(seq_tokens, dtype=jnp.int32)
    cosine, sine = rope_tables(positions)
    queries = rotate(projected[:, :head_width].reshape(head_shape), cosine, sine).astype(
        jnp.bfloat16
    )
    keys = rotate(
        projected[:, head_width : 2 * head_width].reshape(head_shape), cosine, sine
    ).astype(jnp.bfloat16)
    values = projected[:, 2 * head_width :].reshape(head_shape).astype(jnp.bfloat16)
    block_rows = seq_tokens // BLK
    block_count = seq_length // BLK
    first_block = seq_index * block_rows
    key_positions = jnp.arange(seq_length, dtype=jnp.int32)
    chosen_rows = (
        lax.dynamic_slice(layout, (first_block, jnp.int32(0)), (block_rows, block_count)) > 0
    )
    allowed = pair_mask(positions, key_positions, expand_blocks(chosen_rows))
    keys_all, values_all = (
        lax.all_gather(keys, "seq", axis=0, tiled=True),
        lax.all_gather(values, "seq", axis=0, tiled=True),
    )
    scores = (
        jnp.einsum("qhd,khd->hqk", queries, keys_all, preferred_element_type=jnp.float32)
        * score_scale
    )
    scores = jnp.where(allowed[None], scores, MASKED)
    log_norm = jax.nn.logsumexp(scores, axis=2, keepdims=True)
    probs = jnp.exp(scores - log_norm)
    probs_low = probs.astype(jnp.bfloat16)
    attended = jnp.einsum(
        "hqk,khd->qhd", probs_low, values_all, preferred_element_type=jnp.float32
    ).astype(jnp.bfloat16)
    cotangent = incoming.astype(jnp.float32)
    adjoint = cotangent
    gain_grad = jnp.zeros((model_width,), jnp.float32)
    for _ in range(ITERS):
        grad_out = lax.dot_general(
            lax.all_gather(cotangent.astype(jnp.bfloat16), "tensor", axis=0, tiled=True),
            out_weight,
            contract_last,
            preferred_element_type=jnp.float32,
        )
        grad_low = grad_out.astype(jnp.bfloat16).reshape(head_shape)
        delta = jnp.sum(grad_low.astype(jnp.float32) * attended.astype(jnp.float32), axis=2)
        grad_probs = jnp.einsum(
            "qhd,khd->hqk", grad_low, values_all, preferred_element_type=jnp.float32
        )
        grad_scores = (probs * (grad_probs - delta.T[:, :, None])).astype(jnp.bfloat16)
        grad_query = (
            jnp.einsum("hqk,khd->qhd", grad_scores, keys_all, preferred_element_type=jnp.float32)
            * score_scale
        )
        key_part = (
            jnp.einsum("hqk,qhd->khd", grad_scores, queries, preferred_element_type=jnp.float32)
            * score_scale
        )
        value_part = jnp.einsum(
            "hqk,qhd->khd", probs_low, grad_low, preferred_element_type=jnp.float32
        )
        key_grads = lax.psum_scatter(
            jnp.concatenate(
                [
                    key_part.reshape(seq_tokens * lax.axis_size("seq"), head_width),
                    value_part.reshape(seq_tokens * lax.axis_size("seq"), head_width),
                ],
                axis=1,
            ).astype(jnp.bfloat16),
            "seq",
            scatter_dimension=0,
            tiled=True,
        ).astype(jnp.float32)
        grad_key = key_grads[:, :head_width].reshape(head_shape)
        grad_value = key_grads[:, head_width:].reshape(head_shape)
        query_low = (
            rotate_back(grad_query, cosine, sine)
            .astype(jnp.bfloat16)
            .reshape(seq_tokens, head_width)
        )
        key_low = (
            rotate_back(grad_key, cosine, sine).astype(jnp.bfloat16).reshape(seq_tokens, head_width)
        )
        value_low = grad_value.astype(jnp.bfloat16).reshape(seq_tokens, head_width)
        total = lax.dot_general(
            query_low, query_weight, contract_last, preferred_element_type=jnp.float32
        )
        total = total + lax.dot_general(
            key_low, key_weight, contract_last, preferred_element_type=jnp.float32
        )
        total = total + lax.dot_general(
            value_low, value_weight, contract_last, preferred_element_type=jnp.float32
        )
        grad_normed = lax.psum_scatter(
            total.astype(jnp.bfloat16), "tensor", scatter_dimension=0, tiled=True
        ).astype(jnp.float32)
        gain_term = jnp.sum(grad_normed * scaled, axis=0)
        gain_grad = gain_grad + lax.psum(gain_term, ("seq", "tensor"))
        weighted = norm_gain * grad_normed
        inner = jnp.sum(weighted * scaled, axis=1, keepdims=True)
        cotangent = inv_rms * (weighted - scaled * (inner / model_width))
        adjoint = adjoint + cotangent
    return (adjoint, gain_grad * seq_length ** (-0.5))


def xor_pairs(axis, distance):
    return [(i, i ^ distance) for i in range(lax.axis_size(axis))]


def xor_gather(block):
    blocks = {0: block}
    distance = lax.axis_size("tensor") // 2
    while distance:
        for j, held in list(blocks.items()):
            blocks[j ^ distance] = lax.ppermute(
                held, "tensor", xor_pairs("tensor", distance)
            )
        distance //= 2
    return [blocks[j] for j in range(len(blocks))]


def xor_reduce_scatter(blocks):
    held = {j: [block] for j, block in enumerate(blocks)}
    distance = 1
    while distance < lax.axis_size("tensor"):
        for j in [j for j in held if not j & distance]:
            parts = held.pop(j ^ distance)
            if len(parts) > 1:
                parts = [sum(p.astype(jnp.float32) for p in parts).astype(jnp.bfloat16)]
            held[j].append(lax.ppermute(parts[0], "tensor", xor_pairs("tensor", distance)))
        distance *= 2
    return held[0]


def all_sum(values):
    axes = ("seq", "tensor")
    size = lax.axis_size("seq") * lax.axis_size("tensor")
    bits = [1 << i for i in range(size.bit_length() - 1)]
    phases = [bits[:1]] + [bits[i : i + 2] for i in range(1, len(bits), 2)][::-1]
    for phase in phases:
        parts = [values]
        for flips in range(1, 1 << len(phase)):
            distance = sum(bit for i, bit in enumerate(phase) if flips >> i & 1)
            parts.append(lax.ppermute(values, axes, [(i, i ^ distance) for i in range(size)]))
        while len(parts) > 1:
            parts = [x + y for x, y in zip(parts[::2], parts[1::2])]
        values = parts[0]
    return values


def swap(values):
    return lax.all_to_all(values, "seq", split_axis=0, concat_axis=0, tiled=True)


def contract(a, b, da, db):
    return lax.dot_general(
        a, b, (((da,), (db,)), ((), ())), preferred_element_type=jnp.float32
    )


def in_vmem(array):
    return pltpu.with_memory_space_constraint(array, pltpu.VMEM)


def vmem_specs(count):
    return [pl.BlockSpec(memory_space=pltpu.VMEM)] * count


def join_rows(refs, joined):
    rows = refs[0].shape[0]
    for i, ref in enumerate(refs):
        joined[i * rows : (i + 1) * rows, :] = ref[...]


PIECES = 4


def in_hbm(array):
    return pltpu.with_memory_space_constraint(array, pltpu.HBM)


def copies_of(source, target, semaphores):
    rows = source.shape[0] // PIECES
    return [
        pltpu.make_async_copy(
            source.at[pl.ds(j * rows, rows)], target.at[pl.ds(j * rows, rows)], semaphores.at[j]
        )
        for j in range(PIECES)
    ]


def load_kernel(*refs, count):
    copies = []
    for i in range(count):
        copies += copies_of(refs[i], refs[count + i], refs[-1].at[i])
    for copy in copies:
        copy.start()
    for copy in copies:
        copy.wait()


def load(weights):
    size = sum(w.size for w in weights)
    return pl.pallas_call(
        functools.partial(load_kernel, count=len(weights)),
        out_shape=[pltpu.VMEM(w.shape, w.dtype) for w in weights],
        in_specs=[pl.BlockSpec(memory_space=pltpu.HBM)] * len(weights),
        out_specs=vmem_specs(len(weights)),
        scratch_shapes=[pltpu.SemaphoreType.DMA((len(weights), PIECES))],
        compiler_params=pltpu.CompilerParams(vmem_limit_bytes=2**20),
        cost_estimate=pl.CostEstimate(
            flops=256 * size, bytes_accessed=2 * size, transcendentals=0
        ),
    )(*map(in_hbm, weights))


def pull_back_kernel(*refs, pieces):
    terms, (weight_ref, out_ref, joined) = refs[:pieces], refs[pieces:]
    join_rows(terms, joined)
    dests, _, heads, _, width = out_ref.shape
    for index in range(dests * heads):
        grad = contract(joined[...], weight_ref[index * width : (index + 1) * width, :], 1, 1)
        out_ref[index // heads, 0, index % heads] = grad.astype(jnp.bfloat16)


def pull_back(terms, weight, seq):
    rows, model = terms[0].shape
    tokens = rows * len(terms)
    heads = weight.shape[0] // HEAD_DIM
    return pl.pallas_call(
        functools.partial(pull_back_kernel, pieces=len(terms)),
        out_shape=jax.ShapeDtypeStruct((seq, 1, heads // seq, tokens, HEAD_DIM), jnp.bfloat16),
        in_specs=vmem_specs(len(terms) + 1),
        out_specs=vmem_specs(1)[0],
        scratch_shapes=[pltpu.VMEM((tokens, model), jnp.bfloat16)],
        compiler_params=pltpu.CompilerParams(vmem_limit_bytes=8 * 2**20),
        cost_estimate=pl.CostEstimate(
            flops=2 * tokens * weight.size, bytes_accessed=2 * weight.size, transcendentals=0
        ),
    )(*terms, in_vmem(weight))


def project_kernel(*refs, pieces):
    points = refs[:pieces]
    gain_ref, cos_ref, sin_ref, *weights, far_ref = refs[pieces : pieces + 6]
    out_ref, inverse_ref, last_ref, normed, semaphores = refs[pieces + 6 :]
    rows, _ = points[0].shape
    copies = copies_of(far_ref, last_ref, semaphores)
    for copy in copies:
        copy.start()
    for i, ref in enumerate(points):
        point = ref[...].astype(jnp.float32)
        inverse = lax.rsqrt(jnp.mean(point * point, axis=1, keepdims=True) + EPS)
        normed[i * rows : (i + 1) * rows, :] = (gain_ref[...] * (point * inverse)).astype(
            jnp.bfloat16
        )
        inverse_ref[i * rows : (i + 1) * rows, :] = jnp.broadcast_to(
            inverse, (rows, inverse_ref.shape[1])
        )
    dests, _, heads, _, width = out_ref.shape
    group = 2 if dests * heads % 2 == 0 else 1
    for which, weight in enumerate((*weights, last_ref)):
        if which == 2:
            for copy in copies:
                copy.wait()
        for first in range(0, dests * heads, group):
            wide = contract(
                normed[...], weight[:, first * width : (first + group) * width], 1, 0
            )
            for index in range(first, first + group):
                part = wide[:, (index - first) * width : (index - first + 1) * width]
                if which < 2:
                    part = part * cos_ref[...] - pltpu.roll(part, width // 2, 1) * sin_ref[...]
                out_ref[index // heads, which, index % heads] = part.astype(jnp.bfloat16)


def project(points, gain, cosine, sine, weights, seq):
    *weights, last = weights
    rows, model = points[0].shape
    tokens = rows * len(points)
    heads = weights[0].shape[1] // HEAD_DIM
    return pl.pallas_call(
        functools.partial(project_kernel, pieces=len(points)),
        out_shape=[
            jax.ShapeDtypeStruct((seq, 3, heads // seq, tokens, HEAD_DIM), jnp.bfloat16),
            jax.ShapeDtypeStruct((tokens, HEAD_DIM), jnp.float32),
            pltpu.VMEM(last.shape, last.dtype),
        ],
        in_specs=vmem_specs(len(points) + 5) + [pl.BlockSpec(memory_space=pltpu.HBM)],
        out_specs=vmem_specs(3),
        scratch_shapes=[
            pltpu.VMEM((tokens, model), jnp.bfloat16),
            pltpu.SemaphoreType.DMA((PIECES,)),
        ],
        compiler_params=pltpu.CompilerParams(vmem_limit_bytes=12 * 2**20),
        cost_estimate=pl.CostEstimate(
            flops=6 * tokens * weights[0].size,
            bytes_accessed=6 * weights[0].size,
            transcendentals=0,
        ),
    )(*points, gain[None], cosine, sine, *map(in_vmem, weights), in_hbm(last))


def combine_kernel(*refs, pieces, columns):
    points, (inverse_ref, grads_ref, *weights), refs = (
        refs[:pieces], refs[pieces : pieces + 5], refs[pieces + 5 :]
    )
    blocks, gain_ref = refs[:pieces], refs[pieces]
    rows = points[0].shape[0]
    dests, _, heads, width, tokens = grads_ref.shape
    first, last = columns
    step = min(512, last - first)
    for start in range(first, last, step):
        source = slice(start, start + step)
        target = slice(start - first, start - first + step)
        total = sum(
            contract(
                weights[which][source, :],
                grads_ref[:, which].reshape(dests * heads * width, tokens),
                1,
                0,
            )
            for which in range(3)
        )
        low = total.T.astype(jnp.bfloat16)
        gain = jnp.zeros((1, step), jnp.float32)
        for i in range(pieces):
            part = low[i * rows : (i + 1) * rows, :]
            blocks[i][:, target] = part
            scaled = points[i][:, source].astype(jnp.float32) * inverse_ref[
                i * rows : (i + 1) * rows, :1
            ]
            gain = gain + jnp.sum(part.astype(jnp.float32) * scaled, axis=0, keepdims=True)
        gain_ref[:, target] = gain


def combine(points, inverse, grads, weights, columns):
    rows = points[0].shape[0]
    tokens, width = rows * len(points), columns[1] - columns[0]
    *outs, gain = pl.pallas_call(
        functools.partial(combine_kernel, pieces=len(points), columns=columns),
        out_shape=[jax.ShapeDtypeStruct((rows, width), jnp.bfloat16)] * len(points)
        + [jax.ShapeDtypeStruct((1, width), jnp.float32)],
        in_specs=vmem_specs(len(points) + 5),
        out_specs=vmem_specs(len(points) + 1),
        compiler_params=pltpu.CompilerParams(vmem_limit_bytes=8 * 2**20),
        cost_estimate=pl.CostEstimate(
            flops=6 * tokens * width * weights[0].shape[1],
            bytes_accessed=6 * width * weights[0].shape[1],
            transcendentals=0,
        ),
    )(*points, inverse, in_vmem(grads), *map(in_vmem, weights))
    return outs, gain[0]


def advance_kernel(*refs, parts):
    sums, (point_ref, inverse_ref, gain_ref, past_ref, next_ref, total_ref) = (
        refs[: sum(parts)], refs[sum(parts) :]
    )
    rows, model = point_ref.shape
    inverse = inverse_ref[:rows, :1]
    grads, first = [], 0
    for count in parts:
        group = sums[first : first + count]
        grads.append(sum(ref[...].astype(jnp.float32) for ref in group))
        first += count
    edges = [0]
    for grad in grads:
        edges.append(edges[-1] + grad.shape[1])
    spans = [slice(*edge) for edge in zip(edges, edges[1:])]
    scaled = [point_ref[:, s].astype(jnp.float32) * inverse for s in spans]
    weighted = [gain_ref[:, s] * g for s, g in zip(spans, grads)]
    inner = sum(jnp.sum(w * x, axis=1, keepdims=True) for w, x in zip(weighted, scaled))
    for s, w, x in zip(spans, weighted, scaled):
        term = inverse * (w - x * (inner / model))
        next_ref[:, s] = term.astype(jnp.bfloat16)
        total_ref[:, s] = past_ref[:, s].astype(jnp.float32) + term


def advance(sums, point, inverse, gain, past):
    return pl.pallas_call(
        functools.partial(advance_kernel, parts=[len(group) for group in sums]),
        out_shape=[
            jax.ShapeDtypeStruct(point.shape, jnp.bfloat16),
            jax.ShapeDtypeStruct(point.shape, jnp.float32),
        ],
        in_specs=vmem_specs(sum(map(len, sums)) + 4),
        out_specs=vmem_specs(2),
        compiler_params=pltpu.CompilerParams(vmem_limit_bytes=8 * 2**20),
        cost_estimate=pl.CostEstimate(
            flops=16 * point.size, bytes_accessed=16 * point.size, transcendentals=0
        ),
    )(*(p for group in sums for p in group), point, inverse, gain[None], past)


def attention_kernel(
    flip_ref, layout_ref, qkv_ref, g_ref, cos_ref, sin_ref, *refs, step, kept
):
    if kept:
        probs_ref, attended_ref, out_ref, key_acc, value_acc = refs
    else:
        out_ref, probs_ref, attended_ref, key_acc, value_acc = refs
    size, _, heads, rows, width = qkv_ref.shape
    last = g_ref.shape[1] - 1
    tokens = size * rows
    blocks = layout_ref.shape[0]
    flip = flip_ref[0]
    scale = width ** (-0.5)
    half = width // 2

    def turn_back(grad, start, stop):
        turned = jnp.concatenate([grad[half:], -grad[:half]], axis=0)
        cosine = jnp.concatenate([cos_ref[:, start:stop]] * 2, axis=0)
        sine = jnp.concatenate([sin_ref[:, start:stop]] * 2, axis=0)
        return (grad * cosine + turned * sine).astype(jnp.bfloat16)

    def probabilities(keys, query, start, seen):
        key_pos = lax.broadcasted_iota(jnp.int32, (seen, step), 0) ^ flip
        query_pos = (lax.broadcasted_iota(jnp.int32, (seen, step), 1) + start) ^ flip
        key_hot = (
            lax.broadcasted_iota(jnp.int32, (seen, blocks), 1)
            == (lax.broadcasted_iota(jnp.int32, (seen, blocks), 0) ^ flip) // BLK
        )
        query_hot = (
            lax.broadcasted_iota(jnp.int32, (blocks, step), 0)
            == ((lax.broadcasted_iota(jnp.int32, (blocks, step), 1) + start) ^ flip) // BLK
        )
        layout = layout_ref[...].astype(jnp.float32).astype(jnp.bfloat16)
        key_rows = contract(
            key_hot.astype(jnp.float32).astype(jnp.bfloat16), layout, 1, 1
        ).astype(jnp.bfloat16)
        chosen = contract(
            key_rows, query_hot.astype(jnp.float32).astype(jnp.bfloat16), 1, 0
        )
        key_pos, query_pos = key_pos[start:], query_pos[start:]
        key_block, query_block = key_pos // BLK, query_pos // BLK
        near = ((key_block < query_block) & (chosen[start:] > 0.5)) | (
            (key_block == query_block) & (key_pos <= query_pos)
        )
        scores = contract(keys[:seen], query, 1, 1) * scale
        square = jnp.where(near, scores[start:], MASKED)
        if start:
            earlier = jnp.where(chosen[:start] > 0.5, scores[:start], MASKED)
            square = jnp.concatenate([earlier, square], axis=0)
        scores = square
        probs = jnp.exp(scores - jnp.max(scores, axis=0, keepdims=True))
        return probs * (1.0 / jnp.sum(probs, axis=0, keepdims=True))

    for head in range(heads):
        queries, keys, values = (qkv_ref[:, i, head].reshape(tokens, width) for i in range(3))
        grads = g_ref[:, last, head].reshape(tokens, width)
        key_t = keys.T
        key_acc[...] = jnp.zeros_like(key_acc)
        value_acc[...] = jnp.zeros_like(value_acc)

        def write(which, start, stop, value):
            for block in range(start // rows, stop // rows):
                out_ref[block, which, head] = value[
                    :, block * rows - start : (block + 1) * rows - start
                ]

        for start in range(0, tokens, step):
            seen = start + step
            query, grad = queries[start:seen], grads[start:seen]
            if kept:
                probs = probs_ref[head, :seen, start:seen]
            else:
                probs = probabilities(keys, query, start, seen)
                probs_ref[head, :seen, start:seen] = probs
            low = probs.astype(jnp.bfloat16)
            if kept:
                attended = attended_ref[head, :, start:seen]
            else:
                attended = contract(values.T[:, :seen], low, 1, 0).astype(jnp.bfloat16)
                attended_ref[head, :, start:seen] = attended
            delta = jnp.sum(
                attended.astype(jnp.float32) * grad.astype(jnp.float32).T, axis=0, keepdims=True
            )
            grad_probs = contract(values[:seen], grad, 1, 1)
            grad_scores = (probs * (grad_probs - delta)).astype(jnp.bfloat16)
            value_acc[:seen, :] += contract(low, grad, 1, 0)
            key_acc[:seen, :] += contract(grad_scores, query, 1, 0)
            grad_query = contract(key_t[:, :seen], grad_scores, 1, 0) * scale
            write(0, start, seen, turn_back(grad_query, start, seen))
        write(1, 0, tokens, turn_back(key_acc[...].T * scale, 0, tokens))
        write(2, 0, tokens, value_acc[...].T.astype(jnp.bfloat16))


def attention_grads(flip, layout, qkv, grads, cosine, sine, kept=()):
    size, _, heads, rows, width = qkv.shape
    tokens = size * rows
    keep = [
        pltpu.VMEM((heads, tokens, tokens), jnp.float32),
        pltpu.VMEM((heads, width, tokens), jnp.bfloat16),
    ]
    out, *new = pl.pallas_call(
        functools.partial(
            attention_kernel, step=min(max(256, rows), tokens), kept=bool(kept)
        ),
        out_shape=[jax.ShapeDtypeStruct((size, 3, heads, width, rows), jnp.bfloat16)]
        + keep * (not kept),
        in_specs=[pl.BlockSpec(memory_space=pltpu.SMEM)] + vmem_specs(5 + len(kept)),
        out_specs=vmem_specs(1 if kept else 3),
        scratch_shapes=[pltpu.VMEM((tokens, width), jnp.float32)] * 2,
        compiler_params=pltpu.CompilerParams(vmem_limit_bytes=12 * 2**20),
        cost_estimate=pl.CostEstimate(
            flops=heads * 12 * tokens * tokens * width,
            bytes_accessed=heads * 16 * tokens * width,
            transcendentals=0 if kept else heads * tokens * tokens,
        ),
    )(flip, layout, qkv, grads, cosine, sine, *map(in_vmem, kept))
    return out, kept or tuple(new)


def turn_tables(positions):
    freq = THETA ** (-jnp.arange(0, HEAD_DIM, 2, dtype=jnp.float32) / HEAD_DIM)
    angle = freq[:, None] * positions.astype(jnp.float32)[None, :]
    return jnp.cos(angle), jnp.sin(angle)


def swapped_body(
    fixed_point, incoming, norm_gain, query_weight, key_weight, value_weight, out_weight, layout
):
    local_rows, model_width = fixed_point.shape
    seq = lax.axis_size("seq")
    seq_tokens = local_rows * lax.axis_size("tensor")
    seq_length = seq_tokens * seq
    flip = lax.axis_index("tensor") * local_rows
    first = lax.axis_index("seq") * seq_tokens
    *weights, flip, first = lax.optimization_barrier(
        (query_weight, key_weight, out_weight, flip, first)
    )
    *weights, out_weight = load(weights)
    order = jnp.arange(seq_length, dtype=jnp.int32) ^ flip
    cosine, sine = turn_tables(order)
    own_cosine, own_sine = (t[:, 0] for t in rope_tables(order[:seq_tokens] + first))
    half = HEAD_DIM // 2
    own_sine = jnp.concatenate([own_sine[:, :half], -own_sine[:, half:]], axis=1)

    points = xor_gather(fixed_point)
    grad_pieces = xor_gather(incoming)
    sent, inverse, value_weight = project(
        points, norm_gain, own_cosine, own_sine, (*weights, value_weight), seq
    )
    weights = (*weights, value_weight)
    sent = jnp.concatenate([sent, pull_back(grad_pieces, out_weight, seq)], axis=1)
    sent, cosine, sine = lax.optimization_barrier((sent, cosine, sine))
    qkv = grads = swap(sent)

    cotangent = adjoint = incoming
    middle = model_width // 2
    gain_part, kept = jnp.zeros((model_width,), jnp.float32), ()
    for term_index in range(ITERS):
        if term_index:
            grads = swap(pull_back(xor_gather(cotangent), out_weight, seq))
        back, kept = attention_grads(flip[None], layout, qkv, grads, cosine, sine, kept)
        left = swap(back)
        sums, gains = [], []
        for columns in ((0, middle), (middle, model_width)):
            blocks, gain_term = combine(points, inverse, left, weights, columns)
            sums.append(xor_reduce_scatter(blocks))
            gains.append(gain_term)
        gain_part = gain_part + jnp.concatenate(gains)
        cotangent, adjoint = advance(sums, fixed_point, inverse, norm_gain, adjoint)
    return (adjoint, all_sum(gain_part) * seq_length ** (-0.5))


def power_of_two(number):
    return number & (number - 1) == 0


def solution(mesh):
    in_specs = (
        P(("seq", "tensor"), None),
        P(("seq", "tensor"), None),
        P(),
        P(None, "tensor"),
        P(None, "tensor"),
        P(None, "tensor"),
        P("tensor", None),
        P(),
    )
    out_specs = (P(("seq", "tensor"), None), P())
    seq, tensor = mesh.shape["seq"], mesh.shape["tensor"]

    def whole(*arguments):
        local_rows = arguments[0].shape[0] // (seq * tensor)
        heads = arguments[3].shape[1] // (HEAD_DIM * tensor)
        fits = (
            heads % seq == 0
            and all(map(power_of_two, (seq, tensor, local_rows)))
            and local_rows * tensor % BLK == 0
        )
        body = swapped_body if fits else gathered_body
        return jax.shard_map(
            body, mesh=mesh, in_specs=in_specs, out_specs=out_specs, check_vma=False
        )(*arguments)

    return whole
```
